32 devices in a mesh: grp: 4 (over x, core), sub: 8 (over z, y).
Axes of the slice: x: 2, y: 2, z: 4, core: 2. Of those that a mesh axis runs over, the one named last changes fastest.
Arguments:
- fine_res: float32 [3, 131072], P(None, ('grp', 'sub'))
- node_map: int32 [2, 131072], P(None, ('grp', 'sub')), may hold values from 0 to 16383, as said below
- connect: int32 [4, 32768], P(None, 'sub'), may hold values from 0 to 16383, as said below
- grads: float32 [3, 3, 32768], P(None, None, 'sub'), may hold values from -6 to 6
- moduli: float32 [2, 32768], P(None, 'sub'), may hold values from 0.2 to 2
- mass: float32 [16384], P('sub'), may hold values from 0.5 to 4
Outputs:
- correction: float32 [3, 131072], P(None, ('grp', 'sub'))
The draws below stay inside these ranges and needn't reach their ends.
Inputs may be any that keep to these rules, and one draw needn't show every extreme that they name: `node_map`: fine nodes 4096 * b to 4096 * (b + 1) - 1 lie in column c = b % 8; both their entries are coarse nodes c * 2048 to (c + 1) * 2048 - 1 or the first 1024 nodes of column c + 1; the two entries are equal at vertices. `connect`: tetrahedra c * 4096 to (c + 1) * 4096 - 1 lie in column c; their nodes are coarse nodes of column c or the first 1024 nodes of column c + 1.
All inputs are finite; a program needn't handle non-finite values.
Results may differ from the reference program's by a relative error of at most 0.0001.
Values sent between devices are 32-bit elements; how exact they have to be, the bound alone decides.
A program may use at most 64 MiB of HBM per device.

```python
import math
import jax
import jax.numpy as jnp

CN = 2048
CI = 1024
CE = 4096
FN = 4096
ITERS = 3
CNODES = 16384
CELEMS = 32768
FNODES = 131072
N_SUB = 8


def pick_nodes(key, count, column):
    keys = jax.random.split(key, 3)
    own = jax.random.randint(keys[0], (count,), 0, CN, dtype=jnp.int32)
    shared = jax.random.randint(keys[1], (count,), 0, CI, dtype=jnp.int32)
    coin = jax.random.randint(keys[2], (count,), 0, 100, dtype=jnp.int32)
    use_next = (coin < 20) & (column < N_SUB - 1)
    return jnp.where(use_next, (column + 1) * CN + shared, column * CN + own).astype(jnp.int32)


def draw_fine_res(key, part):
    column = jnp.arange(FNODES, dtype=jnp.int32) // FN % N_SUB
    scale = 1.0 + 2.0 * column.astype(jnp.float32) / max(N_SUB - 1, 1)
    values = jax.random.normal(key, (3, FNODES), jnp.float32) * scale[None, :]
    return values


def draw_node_map(key, part):
    column = jnp.arange(FNODES, dtype=jnp.int32) // FN % N_SUB
    keys = jax.random.split(jax.random.fold_in(key, 11), 3)
    first = pick_nodes(keys[0], FNODES, column)
    second = pick_nodes(keys[1], FNODES, column)
    coin = jax.random.randint(keys[2], (FNODES,), 0, 8, dtype=jnp.int32)
    second = jnp.where(coin == 0, first, second)
    return jnp.stack([first, second]).astype(jnp.int32)


def draw_connect(key, part):
    column = jnp.arange(CELEMS, dtype=jnp.int32) // CE
    keys = jax.random.split(jax.random.fold_in(key, 23), 4)
    return jnp.stack([pick_nodes(keys[corner], CELEMS, column) for corner in range(4)]).astype(jnp.int32)


def block_levels(own_key, extent, cuts, low, largest):
    gain, own = 1.0, jax.random.fold_in(own_key, 6)
    for axis_at, shards_of in cuts:
        draws = jnp.exp(jax.random.uniform(jax.random.fold_in(own, axis_at), (shards_of,), jnp.float32, low / len(cuts), largest / len(cuts)))
        gain = gain * jnp.repeat(draws, extent[axis_at] // shards_of).reshape([-1 if axis == axis_at else 1 for axis in range(len(extent))])
    return gain


def normal_values(key, shape, spread, most, shards=(), held_as=jnp.bfloat16):
    drawn = jax.random.normal(key, shape, jnp.float32) * spread
    if len(shards) > 0:
        drawn = block_levels(key, shape, shards, -0.22, 0.18) * drawn
    return jnp.clip(drawn, min=-most, max=most).astype(held_as)


def setup_inputs(seed: int = 0) -> dict:
    streams_of = jax.random.split(jax.random.key(seed), 7)
    fine_res = draw_fine_res(jax.random.fold_in(streams_of[6], 71), 0)
    node_map = draw_node_map(jax.random.fold_in(streams_of[6], 71), 0)
    connect = draw_connect(jax.random.fold_in(streams_of[6], 71), 0)
    grads = normal_values(streams_of[3], (3, 3, CELEMS), 1.0, 6.0, ((2, 8),), jnp.float32)
    moduli = jnp.clip(jnp.exp(math.log(2.0) - 2.3025851 * jax.random.uniform(streams_of[4], (2, CELEMS), jnp.float32) ** block_levels(streams_of[4], (2, CELEMS), ((1, 8),), -0.2, 0.2)), 0.2, 2.0)
    mass = jnp.clip(jnp.exp(math.log(4.0) - 2.0794415 * jax.random.uniform(streams_of[5], (CNODES,), jnp.float32) ** block_levels(streams_of[5], (CNODES,), ((0, 8),), -0.2, 0.2)), 0.5, 4.0)
    return {"fine_res": fine_res, "node_map": node_map, "connect": connect, "grads": grads, "moduli": moduli, "mass": mass}


def element_forces(field, connect, grads, moduli, count):
    last = -(grads[:, 0] + grads[:, 1] + grads[:, 2])
    shape_grads = (grads[:, 0], grads[:, 1], grads[:, 2], last)
    displ_grad = jnp.zeros((3, 3, connect.shape[1]), jnp.float32)
    for corner in range(4):
        moved = jnp.take(field, connect[corner], axis=1)
        displ_grad = displ_grad + moved[:, None, :] * shape_grads[corner][None, :, :]
    strain = 0.5 * (displ_grad + jnp.transpose(displ_grad, (1, 0, 2)))
    trace = strain[0, 0] + strain[1, 1] + strain[2, 2]
    identity = jnp.eye(3, dtype=jnp.float32)[:, :, None]
    stress = 2.0 * moduli[1] * strain + (moduli[0] * trace) * identity
    forces = jnp.zeros((3, count), jnp.float32)
    for corner in range(4):
        nodal = jnp.sum(stress * shape_grads[corner][None, :, :], axis=1)
        forces = forces.at[:, connect[corner]].add(nodal)
    return forces


def operate(field, connect, grads, moduli, mass):
    return mass[None, :] * field + element_forces(field, connect, grads, moduli, field.shape[1])


def reference(fine_res, node_map, connect, grads, moduli, mass):
    total = mass.shape[0]
    half = 0.5 * fine_res
    rhs = jnp.zeros((3, total), jnp.float32).at[:, node_map[0]].add(half).at[:, node_map[1]].add(half)
    solution = jnp.zeros((3, total), jnp.float32)
    residual = rhs
    direction = rhs
    norm_now = jnp.sum(residual * residual)
    for step in range(ITERS):
        image = operate(direction, connect, grads, moduli, mass)
        alpha = norm_now / jnp.sum(direction * image)
        solution = solution + alpha * direction
        residual = residual - alpha * image
        norm_next = jnp.sum(residual * residual)
        direction = residual + (norm_next / norm_now) * direction
        norm_now = norm_next
    return 0.5 * (jnp.take(solution, node_map[0], axis=1) + jnp.take(solution, node_map[1], axis=1))
```

```python
import functools

import jax
import jax.numpy as jnp
from jax import lax
from jax.experimental import pallas as pl
from jax.experimental.pallas import tpu as pltpu
from jax.sharding import PartitionSpec as P

CI = 1024
LANES = 128
TILE = 512
CORES = 2
F32 = jnp.float32
BF16 = jnp.bfloat16
NT = (((1,), (1,)), ((), ()))
MESH = pl.DeviceIdType.MESH


def split(value):
    high = value.astype(BF16)
    return high, (value - high.astype(F32)).astype(BF16)


def hots(index, rows):
    lane = index & (LANES - 1)
    row = index // LANES
    width = index.shape[1]
    lane_hot = jnp.where(lax.broadcasted_iota(jnp.int32, (LANES, width), 0) == lane, 1.0, 0.0).astype(BF16)
    row_hot = lax.broadcasted_iota(jnp.int32, (rows, width), 0) == row
    return lane_hot, row_hot


def pick(parts, lane_hot, row_hot, rows):
    got = jnp.dot(parts, lane_hot, preferred_element_type=F32)
    half = 3 * rows
    got = got[:half] + got[half:]
    return [
        jnp.sum(jnp.where(row_hot, got[d * rows : (d + 1) * rows], 0.0), axis=0, keepdims=True)
        for d in range(3)
    ]


def spread(values, lane_hot, row_hot):
    placed = []
    for value in values:
        placed.append(jnp.where(row_hot, value, 0.0))
    placed = jnp.concatenate(placed, axis=0)
    parts = jnp.concatenate(split(placed), axis=0)
    got = lax.dot_general(parts, lane_hot, NT, preferred_element_type=F32)
    half = got.shape[0] // 2
    return got[:half] + got[half:]


def field_parts(field):
    flat = field.reshape(-1, LANES)
    return jnp.concatenate(split(flat), axis=0)


def folded(row):
    return sum(row[:, at : at + LANES] for at in range(0, row.shape[1], LANES))


def down(value):
    return jnp.sum(value.reshape(-1, LANES), axis=0, keepdims=True)


def whole(row):
    return jnp.sum(row, axis=1, keepdims=True)


class Kernel:
    def __init__(self, refs, rows, nodes, own, shared, groups, columns):
        for name, ref in refs.items():
            setattr(self, name, ref)
        self.rows, self.nodes, self.own, self.shared = rows, nodes, own, shared
        self.groups, self.columns = groups, columns
        self.g = lax.axis_index("grp")
        self.s = lax.axis_index("sub")
        self.core = lax.rem(self.g, CORES)
        self.chip = self.g - self.core
        self.base = self.s * nodes
        self.sent = []
        self.count = 0

    def send(self, src, dst, grp, sub, when=None):
        at = self.count
        self.count += 1
        copy = pltpu.make_async_remote_copy(
            src_ref=src,
            dst_ref=dst,
            send_sem=self.send_sem.at[at],
            recv_sem=self.recv_sem.at[at],
            device_id={"grp": grp, "sub": sub},
            device_id_type=MESH,
        )
        self.guard(when, copy.start)
        self.sent.append((copy, when))
        return copy

    def guard(self, when, act):
        if when is None:
            act()
        else:
            pl.when(when)(act)

    def drain(self):
        for copy, when in self.sent:
            self.guard(when, copy.wait_send)

    def has_next(self):
        return self.s < self.columns - 1

    def has_prev(self):
        return self.s > 0

    def restrict(self):
        total = jnp.zeros((3 * self.rows, LANES), F32)
        for at in range(0, self.fine.shape[1], TILE):
            values = [0.5 * self.fine[d : d + 1, at : at + TILE] for d in range(3)]
            for k in range(2):
                lane_hot, row_hot = hots(self.nmap[k : k + 1, at : at + TILE] - self.base, self.rows)
                total = total + spread(values, lane_hot, row_hot)
        return total.reshape(3, self.rows, LANES)

    def prolong(self, field, out_ref):
        parts = field_parts(field)
        for at in range(0, self.fine.shape[1], TILE):
            both = []
            for k in range(2):
                lane_hot, row_hot = hots(self.nmap[k : k + 1, at : at + TILE] - self.base, self.rows)
                both.append(pick(parts, lane_hot, row_hot, self.rows))
            for d in range(3):
                out_ref[d : d + 1, at : at + TILE] = 0.5 * (both[0][d] + both[1][d])

    def apply(self, field, forces=True, energy=False):
        parts = field_parts(field)
        total = jnp.zeros((3 * self.rows, LANES), F32)
        power = jnp.zeros((1, LANES), F32)
        for at in range(0, self.conn.shape[1], TILE):
            cut = slice(at, at + TILE)
            grad = [[self.grads[i, a : a + 1, cut] for i in range(3)] for a in range(3)]
            grad.append([-(grad[0][i] + grad[1][i] + grad[2][i]) for i in range(3)])
            first = self.moduli[0:1, cut]
            second = self.moduli[1:2, cut]
            hot = [hots(self.conn[a : a + 1, cut] - self.base, self.rows) for a in range(4)]
            moved = [pick(parts, hot[a][0], hot[a][1], self.rows) for a in range(4)]
            h = [[sum(moved[a][i] * grad[a][j] for a in range(4)) for j in range(3)] for i in range(3)]
            bulk = first * (h[0][0] + h[1][1] + h[2][2])
            stress = [[second * (h[i][j] + h[j][i]) for j in range(3)] for i in range(3)]
            for i in range(3):
                stress[i][i] = stress[i][i] + bulk
            if energy:
                power = power + folded(sum(stress[i][j] * h[i][j] for i in range(3) for j in range(3)))
            if forces:
                for a in range(4):
                    nodal = [sum(stress[i][j] * grad[a][j] for j in range(3)) for i in range(3)]
                    total = total + spread(nodal, hot[a][0], hot[a][1])
        return total.reshape(3, self.rows, LANES), power

    def weighted(self, field):
        return 0.5 * self.mass[...][None] * field[:, : self.own]

    def exchange_forces(self, field, forces, phase):
        own, shared, rows = self.own, self.shared, self.rows
        f_ref = self.force.at[phase]
        f_ref[:, :own] = forces[:, :own] + self.weighted(field)
        f_ref[:, own:] = forces[:, own:]
        copies = []
        nxt, prv = self.has_next(), self.has_prev()
        for j in range(CORES):
            grp = self.chip + lax.rem(self.core + j, CORES)
            up = self.send(f_ref.at[:, pl.ds(own, shared)], self.h_prev.at[phase, j], grp, self.s + 1, nxt)
            copies.append((up, prv))
            dn = self.send(f_ref.at[:, pl.ds(0, shared)], self.h_next.at[phase, j], grp, self.s - 1, prv)
            copies.append((dn, nxt))
        grp = self.chip + 1 - self.core
        copies.append((self.send(f_ref, self.h_own.at[phase], grp, self.s), None))
        return copies

    def collect(self, copies):
        for copy, when in copies:
            self.guard(when, copy.wait_recv)

    def join(self, field, before, after):
        own, shared = self.own, self.shared
        return jnp.concatenate(
            [field[:, :shared] + before, field[:, shared:own], field[:, own:] + after], axis=1
        )

    def joined_forces(self, phase):
        both = self.force[phase] + self.h_own[phase]
        return self.join(
            both,
            self.h_prev[phase, 0] + self.h_prev[phase, 1],
            self.h_next[phase, 0] + self.h_next[phase, 1],
        )

    def share(self, buf, value, cores):
        slot = self.s * cores + (self.core if cores > 1 else 0)
        buf[slot] = value
        copies = []
        for k in range(self.columns):
            for j in range(cores):
                if k == 0 and j == 0:
                    continue
                sub = lax.rem(self.s + k, self.columns)
                grp = self.chip + lax.rem(self.core + j, CORES)
                copies.append((self.send(buf.at[slot], buf.at[slot], grp, sub), None))
        return copies

    def run(self):
        own, shared, rows, G = self.own, self.shared, self.rows, self.groups
        g, s = self.g, self.s
        nxt, prv = self.has_next(), self.has_prev()
        barrier = pltpu.get_barrier_semaphore()

        def greet(grp, sub, when=None):
            def act():
                pl.semaphore_signal(barrier, inc=1, device_id={"grp": grp, "sub": sub}, device_id_type=MESH)

            self.guard(when, act)

        for k in range(self.columns):
            for j in range(CORES):
                if k or j:
                    greet(self.chip + lax.rem(self.core + j, CORES), lax.rem(s + k, self.columns))
        for j in range(CORES, G):
            grp = lax.rem(self.chip + j, G)
            greet(grp, s)
            greet(grp, s + 1, nxt)
            greet(grp, s - 1, prv)
        half = self.conn.shape[1]
        at = pl.multiple_of(self.core * half, LANES)
        loads = []
        pairs = [
            (self.nmap_in, self.nmap),
            (self.fine_in, self.fine),
            (self.conn_in.at[:, pl.ds(at, half)], self.conn),
            (self.grads_in.at[:, :, pl.ds(at, half)], self.grads),
            (self.moduli_in.at[:, pl.ds(at, half)], self.moduli),
            (self.mass_in, self.mass),
        ]
        for i, (src, dst) in enumerate(pairs):
            copy = pltpu.make_async_copy(src, dst, self.load_sem.at[i])
            copy.start()
            loads.append(copy)

        @pl.when(jnp.logical_not(prv))
        def _():
            self.r_prev[...] = jnp.zeros_like(self.r_prev)
            self.h_prev[...] = jnp.zeros_like(self.h_prev)

        @pl.when(jnp.logical_not(nxt))
        def _():
            self.r_next[...] = jnp.zeros_like(self.r_next)
            self.h_next[...] = jnp.zeros_like(self.h_next)

        loads[0].wait()
        loads[1].wait()
        self.part[...] = self.restrict()
        far = G - CORES
        pl.semaphore_wait(
            barrier,
            self.columns * CORES - 1 + far + far * (nxt.astype(jnp.int32) + prv.astype(jnp.int32)),
        )
        copies = []
        for j in range(G):
            grp = lax.rem(g + j, G)
            up = self.send(self.part.at[:, pl.ds(own, shared)], self.r_prev.at[j], grp, s + 1, nxt)
            copies.append((up, prv))
            dn = self.send(self.part.at[:, pl.ds(0, shared)], self.r_next.at[j], grp, s - 1, prv)
            copies.append((dn, nxt))
            if j:
                copies.append((self.send(self.part, self.r_own.at[j - 1], grp, s), None))
        for copy in loads[2:]:
            copy.wait()
        self.collect(copies)
        r0 = self.join(
            self.part[...] + sum(self.r_own[j] for j in range(G - 1)),
            sum(self.r_prev[j] for j in range(G)),
            sum(self.r_next[j] for j in range(G)),
        )
        forces, _ = self.apply(r0)
        copies = self.exchange_forces(r0, forces, 0)
        self.prolong(r0, self.back.at[0])
        self.collect(copies)
        w0 = self.joined_forces(0)

        mine, image = r0[:, :own], w0[:, :own]
        first = self.share(
            self.sum1,
            jnp.concatenate([down(mine * mine), down(mine * image), down(image * image), down(image * image)], axis=0),
            1,
        )
        forces, power = self.apply(w0, energy=True)
        second = self.share(self.sum2, power + down(self.weighted(w0) * image), CORES)
        copies = self.exchange_forces(w0, forces, 1)
        self.collect(first)
        sums = sum(self.sum1[i] for i in range(self.columns))
        g0, m1, m2 = sums[0:1], sums[1:2], sums[2:3]
        gamma0, mu1, mu2 = whole(g0), whole(m1), whole(m2)
        alpha0 = gamma0 / mu1
        r1 = r0 - alpha0 * w0
        self.prolong(r1, self.back.at[1])
        self.collect(copies)
        q0 = self.joined_forces(1)
        self.collect(second)
        mu3 = whole(sum(self.sum2[i] for i in range(self.columns * CORES)))
        gamma1 = whole(g0 - 2.0 * alpha0 * m1 + (alpha0 * alpha0) * m2)
        delta1 = mu1 - 2.0 * alpha0 * mu2 + (alpha0 * alpha0) * mu3
        beta1 = gamma1 / gamma0
        alpha1 = gamma1 / (delta1 - beta1 * gamma1 / alpha0)
        r2 = r1 - alpha1 * ((w0 - alpha0 * q0) + beta1 * w0)
        _, power = self.apply(r2, forces=False, energy=True)
        mine = r2[:, :own]
        third = self.share(
            self.sum3,
            jnp.concatenate([0.5 * down(mine * mine), power + down(self.weighted(r2) * mine)], axis=0),
            CORES,
        )
        self.prolong(r2, self.back.at[2])
        self.collect(third)
        sums = sum(self.sum3[i] for i in range(self.columns * CORES))
        gamma2, delta2 = whole(sums[0:1]), whole(sums[1:2])
        beta2 = gamma2 / gamma1
        alpha2 = gamma2 / (delta2 - beta2 * gamma2 / alpha1)
        c1 = alpha1 + alpha2 * beta2
        c0 = alpha0 + beta1 * c1
        self.out[...] = c0 * self.back[0] + c1 * self.back[1] + alpha2 * self.back[2]
        self.drain()


NAMES = (
    "fine_in",
    "nmap_in",
    "conn_in",
    "grads_in",
    "moduli_in",
    "mass_in",
    "out",
    "fine",
    "nmap",
    "conn",
    "grads",
    "moduli",
    "mass",
    "part",
    "r_own",
    "r_prev",
    "r_next",
    "force",
    "h_own",
    "h_prev",
    "h_next",
    "sum1",
    "sum2",
    "sum3",
    "back",
    "load_sem",
    "send_sem",
    "recv_sem",
)


def kernel(*refs, **sizes):
    Kernel(dict(zip(NAMES, refs)), **sizes).run()


def body(groups, columns, fine_res, node_map, connect, grads, moduli, mass):
    nodes = mass.shape[0]
    own = nodes // LANES
    shared = CI // LANES
    rows = own + shared
    half = connect.shape[1] // CORES
    sends = 3 * groups - 1 + 2 * (2 * CORES + 1) + columns - 1 + 2 * (columns * CORES - 1)
    vmem = pltpu.VMEM
    halo = (3, shared, LANES)
    full = (3, rows, LANES)
    return pl.pallas_call(
        functools.partial(
            kernel, rows=rows, nodes=nodes, own=own, shared=shared, groups=groups, columns=columns
        ),
        out_shape=jax.ShapeDtypeStruct(fine_res.shape, F32),
        in_specs=[pl.BlockSpec(memory_space=pl.ANY)] * 6,
        out_specs=pl.BlockSpec(memory_space=vmem),
        scratch_shapes=[
            vmem(fine_res.shape, F32),
            vmem(node_map.shape, jnp.int32),
            vmem((4, half), jnp.int32),
            vmem((3, 3, half), F32),
            vmem((2, half), F32),
            vmem((own, LANES), F32),
            vmem(full, F32),
            vmem((groups - 1,) + full, F32),
            vmem((groups,) + halo, F32),
            vmem((groups,) + halo, F32),
            vmem((2,) + full, F32),
            vmem((2,) + full, F32),
            vmem((2, CORES) + halo, F32),
            vmem((2, CORES) + halo, F32),
            vmem((columns, 4, LANES), F32),
            vmem((columns * CORES, 1, LANES), F32),
            vmem((columns * CORES, 2, LANES), F32),
            vmem((3,) + fine_res.shape, F32),
            pltpu.SemaphoreType.DMA((6,)),
            pltpu.SemaphoreType.DMA((sends,)),
            pltpu.SemaphoreType.DMA((sends,)),
        ],
        compiler_params=pltpu.CompilerParams(
            collective_id=0, has_side_effects=True, vmem_limit_bytes=48 * 1024 * 1024
        ),
    )(fine_res, node_map, connect, grads, moduli, mass.reshape(own, LANES))


def solution(mesh):
    in_specs = (
        P(None, ("grp", "sub")),
        P(None, ("grp", "sub")),
        P(None, "sub"),
        P(None, None, "sub"),
        P(None, "sub"),
        P("sub"),
    )
    out_specs = P(None, ("grp", "sub"))
    return jax.shard_map(
        functools.partial(body, mesh.shape["grp"], mesh.shape["sub"]),
        mesh=mesh,
        in_specs=in_specs,
        out_specs=out_specs,
        check_vma=False,
    )
```

```python
import functools

import jax
import jax.numpy as jnp
from jax import lax
from jax.experimental import pallas as pl
from jax.experimental.pallas import tpu as pltpu
from jax.sharding import PartitionSpec as P

CI = 1024
LANES = 128
TILE = 512
CORES = 2
F32 = jnp.float32
BF16 = jnp.bfloat16
NT = (((1,), (1,)), ((), ()))
MESH = pl.DeviceIdType.MESH


def split(value):
    high = value.astype(BF16)
    return high, (value - high.astype(F32)).astype(BF16)


def hots(index, rows):
    lane = index & (LANES - 1)
    row = index // LANES
    width = index.shape[1]
    lane_hot = jnp.where(lax.broadcasted_iota(jnp.int32, (LANES, width), 0) == lane, 1.0, 0.0).astype(BF16)
    row_hot = lax.broadcasted_iota(jnp.int32, (rows, width), 0) == row
    return lane_hot, row_hot


def pick(parts, lane_hot, row_hot, rows):
    got = jnp.dot(parts, lane_hot, preferred_element_type=F32)
    half = 3 * rows
    got = got[:half] + got[half:]
    return [
        jnp.sum(jnp.where(row_hot, got[d * rows : (d + 1) * rows], 0.0), axis=0, keepdims=True)
        for d in range(3)
    ]


def spread(values, lane_hot, row_hot):
    placed = []
    for value in values:
        placed.append(jnp.where(row_hot, value, 0.0))
    placed = jnp.concatenate(placed, axis=0)
    parts = jnp.concatenate(split(placed), axis=0)
    got = lax.dot_general(parts, lane_hot, NT, preferred_element_type=F32)
    half = got.shape[0] // 2
    return got[:half] + got[half:]


def field_parts(field):
    flat = field.reshape(-1, LANES)
    return jnp.concatenate(split(flat), axis=0)


def folded(row):
    return sum(row[:, at : at + LANES] for at in range(0, row.shape[1], LANES))


def down(value):
    return jnp.sum(value.reshape(-1, LANES), axis=0, keepdims=True)


def whole(row):
    return jnp.sum(row, axis=1, keepdims=True)


class Kernel:
    def __init__(self, refs, rows, nodes, own, shared, groups, columns):
        for name, ref in refs.items():
            setattr(self, name, ref)
        self.rows, self.nodes, self.own, self.shared = rows, nodes, own, shared
        self.groups, self.columns = groups, columns
        self.g = lax.axis_index("grp")
        self.s = lax.axis_index("sub")
        self.core = lax.rem(self.g, CORES)
        self.chip = self.g - self.core
        self.base = self.s * nodes
        self.sent = []
        self.count = 0

    def send(self, src, dst, grp, sub, when=None):
        at = self.count
        self.count += 1
        copy = pltpu.make_async_remote_copy(
            src_ref=src,
            dst_ref=dst,
            send_sem=self.send_sem.at[at],
            recv_sem=self.recv_sem.at[at],
            device_id={"grp": grp, "sub": sub},
            device_id_type=MESH,
        )
        self.guard(when, copy.start)
        self.sent.append((copy, when))
        return copy

    def guard(self, when, act):
        if when is None:
            act()
        else:
            pl.when(when)(act)

    def drain(self):
        for copy, when in self.sent:
            self.guard(when, copy.wait_send)

    def has_next(self):
        return self.s < self.columns - 1

    def has_prev(self):
        return self.s > 0

    def restrict(self):
        total = jnp.zeros((3 * self.rows, LANES), F32)
        for at in range(0, self.fine.shape[1], TILE):
            values = [0.5 * self.fine[d : d + 1, at : at + TILE] for d in range(3)]
            for k in range(2):
                lane_hot, row_hot = hots(self.nmap[k : k + 1, at : at + TILE] - self.base, self.rows)
                total = total + spread(values, lane_hot, row_hot)
        return total.reshape(3, self.rows, LANES)

    def prolong(self, field, out_ref):
        parts = field_parts(field)
        for at in range(0, self.fine.shape[1], TILE):
            both = []
            for k in range(2):
                lane_hot, row_hot = hots(self.nmap[k : k + 1, at : at + TILE] - self.base, self.rows)
                both.append(pick(parts, lane_hot, row_hot, self.rows))
            for d in range(3):
                out_ref[d : d + 1, at : at + TILE] = 0.5 * (both[0][d] + both[1][d])

    def apply(self, field, forces=True, energy=False):
        parts = field_parts(field)
        total = jnp.zeros((3 * self.rows, LANES), F32)
        power = jnp.zeros((1, LANES), F32)
        for at in range(0, self.conn.shape[1], TILE):
            cut = slice(at, at + TILE)
            grad = [[self.grads[i, a : a + 1, cut] for i in range(3)] for a in range(3)]
            grad.append([-(grad[0][i] + grad[1][i] + grad[2][i]) for i in range(3)])
            first = self.moduli[0:1, cut]
            second = self.moduli[1:2, cut]
            hot = [hots(self.conn[a : a + 1, cut] - self.base, self.rows) for a in range(4)]
            moved = [pick(parts, hot[a][0], hot[a][1], self.rows) for a in range(4)]
            h = [[sum(moved[a][i] * grad[a][j] for a in range(4)) for j in range(3)] for i in range(3)]
            bulk = first * (h[0][0] + h[1][1] + h[2][2])
            stress = [[second * (h[i][j] + h[j][i]) for j in range(3)] for i in range(3)]
            for i in range(3):
                stress[i][i] = stress[i][i] + bulk
            if energy:
                power = power + folded(sum(stress[i][j] * h[i][j] for i in range(3) for j in range(3)))
            if forces:
                for a in range(4):
                    nodal = [sum(stress[i][j] * grad[a][j] for j in range(3)) for i in range(3)]
                    total = total + spread(nodal, hot[a][0], hot[a][1])
        return total.reshape(3, self.rows, LANES), power

    def weighted(self, field):
        return 0.5 * self.mass[...][None] * field[:, : self.own]

    def exchange_forces(self, field, forces, phase):
        own, shared, rows = self.own, self.shared, self.rows
        f_ref = self.force.at[phase]
        f_ref[:, :own] = forces[:, :own] + self.weighted(field)
        f_ref[:, own:] = forces[:, own:]
        copies = []
        nxt, prv = self.has_next(), self.has_prev()
        for j in range(CORES):
            grp = self.chip + lax.rem(self.core + j, CORES)
            up = self.send(f_ref.at[:, pl.ds(own, shared)], self.h_prev.at[phase, j], grp, self.s + 1, nxt)
            copies.append((up, prv))
            dn = self.send(f_ref.at[:, pl.ds(0, shared)], self.h_next.at[phase, j], grp, self.s - 1, prv)
            copies.append((dn, nxt))
        grp = self.chip + 1 - self.core
        copies.append((self.send(f_ref, self.h_own.at[phase], grp, self.s), None))
        return copies

    def collect(self, copies):
        for copy, when in copies:
            self.guard(when, copy.wait_recv)

    def join(self, field, before, after):
        own, shared = self.own, self.shared
        return jnp.concatenate(
            [field[:, :shared] + before, field[:, shared:own], field[:, own:] + after], axis=1
        )

    def joined_forces(self, phase):
        both = self.force[phase] + self.h_own[phase]
        return self.join(
            both,
            self.h_prev[phase, 0] + self.h_prev[phase, 1],
            self.h_next[phase, 0] + self.h_next[phase, 1],
        )

    def share(self, buf, value, cores):
        slot = self.s * cores + (self.core if cores > 1 else 0)
        buf[slot] = value
        copies = []
        for k in range(self.columns):
            for j in range(cores):
                if k == 0 and j == 0:
                    continue
                sub = lax.rem(self.s + k, self.columns)
                grp = self.chip + lax.rem(self.core + j, CORES)
                copies.append((self.send(buf.at[slot], buf.at[slot], grp, sub), None))
        return copies

    def run(self):
        own, shared, rows, G = self.own, self.shared, self.rows, self.groups
        g, s = self.g, self.s
        nxt, prv = self.has_next(), self.has_prev()
        barrier = pltpu.get_barrier_semaphore()

        def greet(grp, sub, when=None):
            def act():
                pl.semaphore_signal(barrier, inc=1, device_id={"grp": grp, "sub": sub}, device_id_type=MESH)

            self.guard(when, act)

        for k in range(self.columns):
            for j in range(CORES):
                if k or j:
                    greet(self.chip + lax.rem(self.core + j, CORES), lax.rem(s + k, self.columns))
        for j in range(CORES, G):
            grp = lax.rem(self.chip + j, G)
            greet(grp, s)
            greet(grp, s + 1, nxt)
            greet(grp, s - 1, prv)
        half = self.conn.shape[1]
        at = pl.multiple_of(self.core * half, LANES)
        loads = []
        pairs = [
            (self.nmap_in, self.nmap),
            (self.fine_in, self.fine),
            (self.conn_in.at[:, pl.ds(at, half)], self.conn),
            (self.grads_in.at[:, :, pl.ds(at, half)], self.grads),
            (self.moduli_in.at[:, pl.ds(at, half)], self.moduli),
            (self.mass_in, self.mass),
        ]
        for i, (src, dst) in enumerate(pairs):
            copy = pltpu.make_async_copy(src, dst, self.load_sem.at[i])
            copy.start()
            loads.append(copy)

        @pl.when(jnp.logical_not(prv))
        def _():
            self.r_prev[...] = jnp.zeros_like(self.r_prev)
            self.h_prev[...] = jnp.zeros_like(self.h_prev)

        @pl.when(jnp.logical_not(nxt))
        def _():
            self.r_next[...] = jnp.zeros_like(self.r_next)
            self.h_next[...] = jnp.zeros_like(self.h_next)

        loads[0].wait()
        loads[1].wait()
        self.part[...] = self.restrict()
        far = G - CORES
        pl.semaphore_wait(
            barrier,
            self.columns * CORES - 1 + far + far * (nxt.astype(jnp.int32) + prv.astype(jnp.int32)),
        )
        copies = []
        for j in range(G):
            grp = lax.rem(g + j, G)
            up = self.send(self.part.at[:, pl.ds(own, shared)], self.r_prev.at[j], grp, s + 1, nxt)
            copies.append((up, prv))
            dn = self.send(self.part.at[:, pl.ds(0, shared)], self.r_next.at[j], grp, s - 1, prv)
            copies.append((dn, nxt))
            if j:
                copies.append((self.send(self.part, self.r_own.at[j - 1], grp, s), None))
        for copy in loads[2:]:
            copy.wait()
        self.collect(copies)
        r0 = self.join(
            self.part[...] + sum(self.r_own[j] for j in range(G - 1)),
            sum(self.r_prev[j] for j in range(G)),
            sum(self.r_next[j] for j in range(G)),
        )
        forces, _ = self.apply(r0)
        copies = self.exchange_forces(r0, forces, 0)
        self.prolong(r0, self.back.at[0])
        self.collect(copies)
        w0 = self.joined_forces(0)

        mine, image = r0[:, :own], w0[:, :own]
        first = self.share(
            self.sum1,
            jnp.concatenate([down(mine * mine), down(mine * image), down(image * image), down(image * image)], axis=0),
            1,
        )
        forces, power = self.apply(w0, energy=True)
        second = self.share(self.sum2, power + down(self.weighted(w0) * image), CORES)
        copies = self.exchange_forces(w0, forces, 1)
        self.collect(first)
        sums = sum(self.sum1[i] for i in range(self.columns))
        g0, m1, m2 = sums[0:1], sums[1:2], sums[2:3]
        gamma0, mu1, mu2 = whole(g0), whole(m1), whole(m2)
        alpha0 = gamma0 / mu1
        r1 = r0 - alpha0 * w0
        self.collect(copies)
        q0 = self.joined_forces(1)
        self.collect(second)
        mu3 = whole(sum(self.sum2[i] for i in range(self.columns * CORES)))
        gamma1 = whole(g0 - 2.0 * alpha0 * m1 + (alpha0 * alpha0) * m2)
        delta1 = mu1 - 2.0 * alpha0 * mu2 + (alpha0 * alpha0) * mu3
        beta1 = gamma1 / gamma0
        alpha1 = gamma1 / (delta1 - beta1 * gamma1 / alpha0)
        r2 = r1 - alpha1 * ((w0 - alpha0 * q0) + beta1 * w0)
        _, power = self.apply(r2, forces=False, energy=True)
        mine = r2[:, :own]
        third = self.share(
            self.sum3,
            jnp.concatenate([0.5 * down(mine * mine), power + down(self.weighted(r2) * mine)], axis=0),
            CORES,
        )
        self.prolong(r1, self.back.at[1])
        self.prolong(r2, self.back.at[2])
        self.collect(third)
        sums = sum(self.sum3[i] for i in range(self.columns * CORES))
        gamma2, delta2 = whole(sums[0:1]), whole(sums[1:2])
        beta2 = gamma2 / gamma1
        alpha2 = gamma2 / (delta2 - beta2 * gamma2 / alpha1)
        c1 = alpha1 + alpha2 * beta2
        c0 = alpha0 + beta1 * c1
        self.out[...] = c0 * self.back[0] + c1 * self.back[1] + alpha2 * self.back[2]
        self.drain()


NAMES = (
    "fine_in",
    "nmap_in",
    "conn_in",
    "grads_in",
    "moduli_in",
    "mass_in",
    "out",
    "fine",
    "nmap",
    "conn",
    "grads",
    "moduli",
    "mass",
    "part",
    "r_own",
    "r_prev",
    "r_next",
    "force",
    "h_own",
    "h_prev",
    "h_next",
    "sum1",
    "sum2",
    "sum3",
    "back",
    "load_sem",
    "send_sem",
    "recv_sem",
)


def kernel(*refs, **sizes):
    Kernel(dict(zip(NAMES, refs)), **sizes).run()


def body(groups, columns, fine_res, node_map, connect, grads, moduli, mass):
    nodes = mass.shape[0]
    own = nodes // LANES
    shared = CI // LANES
    rows = own + shared
    half = connect.shape[1] // CORES
    sends = 3 * groups - 1 + 2 * (2 * CORES + 1) + columns - 1 + 2 * (columns * CORES - 1)
    vmem = pltpu.VMEM
    arrays = (fine_res, node_map, connect, grads, moduli, mass.reshape(own, LANES))
    halo = (3, shared, LANES)
    full = (3, rows, LANES)
    return pl.pallas_call(
        functools.partial(
            kernel, rows=rows, nodes=nodes, own=own, shared=shared, groups=groups, columns=columns
        ),
        out_shape=jax.ShapeDtypeStruct(fine_res.shape, F32),
        in_specs=[pl.BlockSpec(memory_space=pltpu.HBM)] * 6,
        out_specs=pl.BlockSpec(memory_space=vmem),
        scratch_shapes=[
            vmem(fine_res.shape, F32),
            vmem(node_map.shape, jnp.int32),
            vmem((4, half), jnp.int32),
            vmem((3, 3, half), F32),
            vmem((2, half), F32),
            vmem((own, LANES), F32),
            vmem(full, F32),
            vmem((groups - 1,) + full, F32),
            vmem((groups,) + halo, F32),
            vmem((groups,) + halo, F32),
            vmem((2,) + full, F32),
            vmem((2,) + full, F32),
            vmem((2, CORES) + halo, F32),
            vmem((2, CORES) + halo, F32),
            vmem((columns, 4, LANES), F32),
            vmem((columns * CORES, 1, LANES), F32),
            vmem((columns * CORES, 2, LANES), F32),
            vmem((3,) + fine_res.shape, F32),
            pltpu.SemaphoreType.DMA((6,)),
            pltpu.SemaphoreType.DMA((sends,)),
            pltpu.SemaphoreType.DMA((sends,)),
        ],
        compiler_params=pltpu.CompilerParams(
            collective_id=0, has_side_effects=True, vmem_limit_bytes=48 * 1024 * 1024
        ),
    )(*[pltpu.with_memory_space_constraint(x, pltpu.HBM) for x in arrays])


def solution(mesh):
    in_specs = (
        P(None, ("grp", "sub")),
        P(None, ("grp", "sub")),
        P(None, "sub"),
        P(None, None, "sub"),
        P(None, "sub"),
        P("sub"),
    )
    out_specs = P(None, ("grp", "sub"))
    return jax.shard_map(
        functools.partial(body, mesh.shape["grp"], mesh.shape["sub"]),
        mesh=mesh,
        in_specs=in_specs,
        out_specs=out_specs,
        check_vma=False,
    )
```

```python
import functools

import jax
import jax.numpy as jnp
from jax import lax
from jax.experimental import pallas as pl
from jax.experimental.pallas import tpu as pltpu
from jax.sharding import PartitionSpec as P

CI = 1024
LANES = 128
TILE = 512
SUB = 8
CORES = 2
F32 = jnp.float32
BF16 = jnp.bfloat16
NT = (((1,), (1,)), ((), ()))
MESH = pl.DeviceIdType.MESH


def lane_hots(index):
    wide = lax.broadcasted_iota(jnp.int32, (LANES, index.shape[1]), 0)
    return jnp.where(wide == (index & (LANES - 1)), 1.0, 0.0).astype(BF16)


def turned_hots(index):
    square = (LANES, LANES)
    turned = jnp.transpose(jnp.broadcast_to(index & (LANES - 1), square))
    return jnp.where(lax.broadcasted_iota(jnp.int32, square, 1) == turned, 1.0, 0.0).astype(BF16)


def row_hots(index, rows):
    wide = lax.broadcasted_iota(jnp.int32, (2 * rows, index.shape[1]), 0)
    wide = wide // (2 * SUB) * SUB + (wide & (SUB - 1))
    return jnp.where(wide == index // LANES, 1.0, 0.0).astype(BF16)


def twice(value):
    high = value.astype(BF16).astype(F32)
    return high, value - high


def stacked(high, low):
    shape = (SUB, high.shape[1])
    both = jnp.concatenate([jnp.broadcast_to(high, shape), jnp.broadcast_to(low, shape)], axis=0)
    return both.astype(BF16)


def placed(values, row_hot):
    parts = []
    for value in values:
        for at in range(0, row_hot.shape[0], 2 * SUB):
            parts.append(row_hot[at : at + 2 * SUB] * value)
    return jnp.concatenate(parts, axis=0)


def merged(total, rows):
    total = total.reshape(3 * rows // SUB, 2, SUB, LANES)
    return (total[:, 0] + total[:, 1]).reshape(3, rows, LANES)


def gather(ref, lane, row):
    found = [jnp.zeros((SUB, LANES), F32) for _ in range(3)]
    for r in range(ref.shape[1]):
        here = row == r
        for d in range(3):
            line = jnp.broadcast_to(ref[d, r : r + 1, :], (SUB, LANES))
            found[d] = jnp.where(here, jnp.take_along_axis(line, lane, axis=1), found[d])
    return found


def down(value):
    return jnp.sum(value.reshape(-1, LANES), axis=0, keepdims=True)


def whole(row):
    return jnp.sum(row, axis=1, keepdims=True)


class Kernel:
    def __init__(self, refs, rows, nodes, own, shared, groups, columns):
        for name, ref in refs.items():
            setattr(self, name, ref)
        self.rows, self.nodes, self.own, self.shared = rows, nodes, own, shared
        self.groups, self.columns = groups, columns
        self.g = lax.axis_index("grp")
        self.s = lax.axis_index("sub")
        self.core = lax.rem(self.g, CORES)
        self.chip = self.g - self.core
        self.base = self.s * nodes
        self.sent = []
        self.count = 0

    def send(self, src, dst, grp, sub, when=None):
        at = self.count
        self.count += 1
        copy = pltpu.make_async_remote_copy(
            src_ref=src,
            dst_ref=dst,
            send_sem=self.send_sem.at[at],
            recv_sem=self.recv_sem.at[at],
            device_id={"grp": grp, "sub": sub},
            device_id_type=MESH,
        )
        self.guard(when, copy.start)
        self.sent.append((copy, when))
        return copy

    def guard(self, when, act):
        if when is None:
            act()
        else:
            pl.when(when)(act)

    def drain(self):
        for copy, when in self.sent:
            self.guard(when, copy.wait_send)
        self.sent = []

    def has_next(self):
        return self.s < self.columns - 1

    def has_prev(self):
        return self.s > 0

    def restrict(self):
        total = jnp.zeros((6 * self.rows, LANES), F32)
        for at in range(0, self.fine.shape[1], TILE):
            values = [stacked(*twice(0.5 * self.fine[d : d + 1, at : at + TILE])) for d in range(3)]
            for k in range(2):
                index = self.nmap[k : k + 1, at : at + TILE] - self.base
                left = placed(values, row_hots(index, self.rows))
                total = total + lax.dot_general(left, lane_hots(index), NT, preferred_element_type=F32)
        return merged(total, self.rows)

    def densify(self):
        for at in range(0, self.fine.shape[1], LANES):
            j = at // LANES
            for k in range(2):
                self.nmap_d[k, j : j + 1] = self.nmap[k : k + 1, at : at + LANES] - self.base
        for at in range(0, self.conn.shape[1], LANES):
            j, cut = at // LANES, slice(at, at + LANES)
            for a in range(4):
                self.conn_d[a, j : j + 1] = self.conn[a : a + 1, cut] - self.base
            for k in range(2):
                self.moduli_d[k, j : j + 1] = self.moduli[k : k + 1, cut]
            for i in range(3):
                line = [self.grads[i, a : a + 1, cut] for a in range(3)]
                for a in range(3):
                    self.grads_d[a, i, j : j + 1] = line[a]
                self.grads_d[3, i, j : j + 1] = -(line[0] + line[1] + line[2])

    def make_hots(self):
        width = self.conn.shape[1]
        for a in range(4):
            for at in range(0, width, TILE):
                index = self.conn[a : a + 1, at : at + TILE] - self.base
                for more in range(0, TILE, LANES):
                    start = a * width + at + more
                    self.lane_hot[start : start + LANES] = turned_hots(index[:, more : more + LANES])
                self.row_hot[:, a * width + at : a * width + at + TILE] = row_hots(index, self.rows)

    def prolong(self, field, out_ref):
        for j in range(0, self.nmap_d.shape[1], SUB):
            both = []
            for k in range(2):
                index = self.nmap_d[k, j : j + SUB]
                both.append(gather(field, index & (LANES - 1), index // LANES))
            for d in range(3):
                mean = 0.5 * (both[0][d] + both[1][d])
                for i in range(SUB):
                    out_ref[d : d + 1, (j + i) * LANES : (j + i + 1) * LANES] = mean[i : i + 1]

    def slopes(self, field, j, slot):
        cut = slice(j, j + SUB)
        grad = [[self.grads_d[a, i, cut] for i in range(3)] for a in range(4)]
        moved = []
        for a in range(4):
            index = self.conn_d[a, cut]
            moved.append(gather(field, index & (LANES - 1), index // LANES))
        h = [[sum(moved[a][i] * grad[a][k] for a in range(4)) for k in range(3)] for i in range(3)]
        for i in range(3):
            for k in range(3):
                self.slope[slot, i, k, cut] = h[i][k]
        return h, grad

    def stresses(self, h, j):
        first = self.moduli_d[0, j : j + SUB]
        second = self.moduli_d[1, j : j + SUB]
        bulk = first * (h[0][0] + h[1][1] + h[2][2])
        stress = [[second * (h[i][k] + h[k][i]) for k in range(3)] for i in range(3)]
        for i in range(3):
            stress[i][i] = stress[i][i] + bulk
        return stress, sum(stress[i][k] * h[i][k] for i in range(3) for k in range(3))

    def strains(self, field, j, slot):
        h, grad = self.slopes(field, j, slot)
        stress, power = self.stresses(h, j)
        nodal = []
        for a in range(4):
            nodal.append([twice(sum(stress[i][k] * grad[a][k] for k in range(3))) for i in range(3)])
        return power, nodal

    def blocks(self):
        return range(0, self.conn_d.shape[1], SUB)

    def energy(self, c1, c2):
        total = jnp.zeros((SUB, LANES), F32)
        for j in self.blocks():
            cut = slice(j, j + SUB)
            h = [
                [
                    self.slope[0, i, k, cut] - c1 * self.slope[1, i, k, cut] + c2 * self.slope[2, i, k, cut]
                    for k in range(3)
                ]
                for i in range(3)
            ]
            total = total + self.stresses(h, j)[1]
        return down(total)

    def hold(self, nodal, block):
        cut = slice(block, block + SUB)
        for a in range(4):
            for d in range(3):
                for k in range(2):
                    self.nodal[a, d, k, cut] = nodal[a][d][k]

    def spread(self, block, total):
        width = self.conn.shape[1]
        tile = TILE // LANES
        for a in range(4):
            for at in range(block, block + SUB, tile):
                values = []
                for d in range(3):
                    high, low = self.nodal.at[a, d, 0], self.nodal.at[a, d, 1]
                    pieces = [stacked(high[j : j + 1], low[j : j + 1]) for j in range(at, at + tile)]
                    values.append(jnp.concatenate(pieces, axis=1))
                cut = slice(a * width + at * LANES, a * width + at * LANES + TILE)
                left = placed(values, self.row_hot[:, cut])
                total = total + jnp.dot(left, self.lane_hot[cut], preferred_element_type=F32)
        return total

    def apply(self, field, slot, between=None):
        total = jnp.zeros((6 * self.rows, LANES), F32)
        power, held = None, None
        for block in self.blocks():
            more, nodal = self.strains(field, block, slot)
            power = more if power is None else power + more
            self.hold(nodal, block)
            if held is not None:
                total = self.spread(held, total)
            held = block
        extra = None if between is None else between(down(power))
        return merged(self.spread(held, total), self.rows), extra

    def weighted(self, field):
        return 0.5 * self.mass[...][None] * field[:, : self.own]

    def exchange_forces(self, field, forces, phase):
        own, shared, rows = self.own, self.shared, self.rows
        f_ref = self.force.at[phase]
        f_ref[:, :own] = forces[:, :own] + self.weighted(field)
        f_ref[:, own:] = forces[:, own:]
        copies = []
        nxt, prv = self.has_next(), self.has_prev()
        for j in range(CORES):
            grp = self.chip + lax.rem(self.core + j, CORES)
            up = self.send(f_ref.at[:, pl.ds(own, shared)], self.h_prev.at[phase, j], grp, self.s + 1, nxt)
            copies.append((up, prv))
            dn = self.send(f_ref.at[:, pl.ds(0, shared)], self.h_next.at[phase, j], grp, self.s - 1, prv)
            copies.append((dn, nxt))
        grp = self.chip + 1 - self.core
        copies.append((self.send(f_ref, self.h_own.at[phase], grp, self.s), None))
        return copies

    def collect(self, copies):
        for copy, when in copies:
            self.guard(when, copy.wait_recv)

    def join(self, field, before, after):
        own, shared = self.own, self.shared
        return jnp.concatenate(
            [field[:, :shared] + before, field[:, shared:own], field[:, own:] + after], axis=1
        )

    def joined_forces(self, phase):
        both = self.force[phase] + self.h_own[phase]
        return self.join(
            both,
            self.h_prev[phase, 0] + self.h_prev[phase, 1],
            self.h_next[phase, 0] + self.h_next[phase, 1],
        )

    def share(self, buf, value):
        slot = self.s * CORES + self.core
        buf[slot] = value
        copies = []
        for k in range(self.columns):
            for j in range(CORES):
                if k or j:
                    sub = lax.rem(self.s + k, self.columns)
                    grp = self.chip + lax.rem(self.core + j, CORES)
                    copies.append((self.send(buf.at[slot], buf.at[slot], grp, sub), None))
        return copies

    def total(self, buf):
        return sum(buf[i] for i in range(self.columns * CORES))

    def run(self):
        own, shared, rows, G = self.own, self.shared, self.rows, self.groups
        g, s = self.g, self.s
        nxt, prv = self.has_next(), self.has_prev()
        half = self.conn.shape[1]
        at = pl.multiple_of(self.core * half, LANES)
        loads = []
        pairs = [
            (self.nmap_in, self.nmap),
            (self.fine_in, self.fine),
            (self.conn_in.at[:, pl.ds(at, half)], self.conn),
            (self.grads_in.at[:, :, pl.ds(at, half)], self.grads),
            (self.moduli_in.at[:, pl.ds(at, half)], self.moduli),
            (self.mass_in, self.mass),
        ]
        for i, (src, dst) in enumerate(pairs):
            copy = pltpu.make_async_copy(src, dst, self.load_sem.at[i])
            copy.start()
            loads.append(copy)

        barrier = pltpu.get_barrier_semaphore()

        def greet(grp, sub, when=None):
            def act():
                pl.semaphore_signal(barrier, inc=1, device_id={"grp": grp, "sub": sub}, device_id_type=MESH)

            self.guard(when, act)

        ends = self.columns >= 8
        edge = jnp.logical_or(s < 2, s >= self.columns - 2)
        for k in range(self.columns):
            sub = lax.rem(s + k, self.columns)
            meets = None
            if ends and k:
                meets = jnp.logical_not(jnp.logical_and(edge, s + sub == self.columns - 1))
            for j in range(CORES):
                if k or j:
                    greet(self.chip + lax.rem(self.core + j, CORES), sub, meets)
        for j in range(CORES, G):
            grp = lax.rem(self.chip + j, G)
            greet(grp, s)
            greet(grp, s + 1, nxt)
            greet(grp, s - 1, prv)

        @pl.when(jnp.logical_not(prv))
        def _():
            self.r_prev[...] = jnp.zeros_like(self.r_prev)
            self.h_prev[...] = jnp.zeros_like(self.h_prev)

        @pl.when(jnp.logical_not(nxt))
        def _():
            self.r_next[...] = jnp.zeros_like(self.r_next)
            self.h_next[...] = jnp.zeros_like(self.h_next)

        loads[0].wait()
        loads[1].wait()
        self.part[...] = self.restrict()
        far = G - CORES
        missed = edge.astype(jnp.int32) if ends else 0
        pl.semaphore_wait(
            barrier,
            self.columns * CORES - 1 - CORES * missed + far + far * (nxt.astype(jnp.int32) + prv.astype(jnp.int32)),
        )
        copies = []
        for j in range(G):
            grp = lax.rem(g + j, G)
            up = self.send(self.part.at[:, pl.ds(own, shared)], self.r_prev.at[j], grp, s + 1, nxt)
            copies.append((up, prv))
            dn = self.send(self.part.at[:, pl.ds(0, shared)], self.r_next.at[j], grp, s - 1, prv)
            copies.append((dn, nxt))
            if j:
                copies.append((self.send(self.part, self.r_own.at[j - 1], grp, s), None))
        for copy in loads[2:]:
            copy.wait()
        self.densify()
        self.make_hots()
        self.collect(copies)
        r0 = self.join(
            self.part[...] + sum(self.r_own[j] for j in range(G - 1)),
            sum(self.r_prev[j] for j in range(G)),
            sum(self.r_next[j] for j in range(G)),
        )
        self.res[0] = r0
        forces, _ = self.apply(self.res.at[0], 0)
        copies = self.exchange_forces(r0, forces, 0)
        self.prolong(self.res.at[0], self.back.at[0])
        self.collect(copies)
        w0 = self.joined_forces(0)
        self.image[...] = w0
        mine, image = 0.5 * r0[:, :own], w0[:, :own]
        lines = [down(mine * r0[:, :own]), down(mine * image), down(0.5 * image * image)]
        weight = down(self.weighted(w0) * image)

        def early(power):
            return self.share(self.sum1, jnp.concatenate(lines + [power + weight], axis=0))

        forces, shares = self.apply(self.image, 1, early)
        copies = self.exchange_forces(w0, forces, 1)
        self.collect(copies)
        q0 = self.joined_forces(1)
        self.twin[...] = q0
        for j in self.blocks():
            self.slopes(self.twin, j, 2)
        self.collect(shares)
        sums = self.total(self.sum1)
        means = whole(sums)
        gamma0, mu1, mu2, mu3 = (means[i : i + 1] for i in range(4))
        alpha0 = gamma0 / mu1
        square = alpha0 * alpha0
        gamma1 = whole(sums[0:1] - 2.0 * alpha0 * sums[1:2] + square * sums[2:3])
        delta1 = mu1 - 2.0 * alpha0 * mu2 + square * mu3
        beta1 = gamma1 / gamma0
        alpha1 = gamma1 / (delta1 - beta1 * gamma1 / alpha0)
        a, b = alpha0 + alpha1 + alpha1 * beta1, alpha1 * alpha0
        r2 = r0 - a * w0 + b * q0
        mine = r2[:, :own]
        lines = [down(0.5 * mine * mine), down(self.weighted(r2) * mine) + self.energy(a, b)]
        shares = self.share(self.sum2, jnp.concatenate(lines, axis=0))
        self.res[1] = r0 - alpha0 * w0
        self.res[2] = r2
        self.prolong(self.res.at[1], self.back.at[1])
        self.prolong(self.res.at[2], self.back.at[2])
        self.drain()
        over_gamma, over_alpha = 1.0 / gamma1, 1.0 / alpha1
        self.collect(shares)
        means = whole(self.total(self.sum2))
        gamma2, delta2 = means[0:1], means[1:2]
        beta2 = gamma2 * over_gamma
        alpha2 = gamma2 / (delta2 - beta2 * (gamma2 * over_alpha))
        c1 = alpha1 + alpha2 * beta2
        c0 = alpha0 + beta1 * c1
        self.out[...] = c0 * self.back[0] + c1 * self.back[1] + alpha2 * self.back[2]


NAMES = (
    "fine_in",
    "nmap_in",
    "conn_in",
    "grads_in",
    "moduli_in",
    "mass_in",
    "out",
    "fine",
    "nmap",
    "conn",
    "grads",
    "moduli",
    "mass",
    "part",
    "r_own",
    "r_prev",
    "r_next",
    "force",
    "h_own",
    "h_prev",
    "h_next",
    "sum1",
    "sum2",
    "back",
    "res",
    "image",
    "twin",
    "slope",
    "nmap_d",
    "conn_d",
    "grads_d",
    "moduli_d",
    "nodal",
    "lane_hot",
    "row_hot",
    "load_sem",
    "send_sem",
    "recv_sem",
)


def kernel(*refs, **sizes):
    Kernel(dict(zip(NAMES, refs)), **sizes).run()


def body(groups, columns, fine_res, node_map, connect, grads, moduli, mass):
    nodes = mass.shape[0]
    own = nodes // LANES
    shared = CI // LANES
    rows = own + shared
    half = connect.shape[1] // CORES
    sends = 3 * groups - 1 + 2 * (2 * CORES + 1) + 2 * (columns * CORES - 1)
    vmem = pltpu.VMEM
    arrays = (fine_res, node_map, connect, grads, moduli, mass.reshape(own, LANES))
    halo = (3, shared, LANES)
    full = (3, rows, LANES)
    return pl.pallas_call(
        functools.partial(
            kernel, rows=rows, nodes=nodes, own=own, shared=shared, groups=groups, columns=columns
        ),
        out_shape=jax.ShapeDtypeStruct(fine_res.shape, F32),
        in_specs=[pl.BlockSpec(memory_space=pltpu.HBM)] * 6,
        out_specs=pl.BlockSpec(memory_space=vmem),
        scratch_shapes=[
            vmem(fine_res.shape, F32),
            vmem(node_map.shape, jnp.int32),
            vmem((4, half), jnp.int32),
            vmem((3, 3, half), F32),
            vmem((2, half), F32),
            vmem((own, LANES), F32),
            vmem(full, F32),
            vmem((groups - 1,) + full, F32),
            vmem((groups,) + halo, F32),
            vmem((groups,) + halo, F32),
            vmem((2,) + full, F32),
            vmem((2,) + full, F32),
            vmem((2, CORES) + halo, F32),
            vmem((2, CORES) + halo, F32),
            vmem((columns * CORES, 4, LANES), F32),
            vmem((columns * CORES, 2, LANES), F32),
            vmem((3,) + fine_res.shape, F32),
            vmem((3,) + full, F32),
            vmem(full, F32),
            vmem(full, F32),
            vmem((3, 3, 3, half // LANES, LANES), F32),
            vmem((2, node_map.shape[1] // LANES, LANES), jnp.int32),
            vmem((4, half // LANES, LANES), jnp.int32),
            vmem((4, 3, half // LANES, LANES), F32),
            vmem((2, half // LANES, LANES), F32),
            vmem((4, 3, 2, half // LANES, LANES), F32),
            vmem((4 * half, LANES), BF16),
            vmem((2 * rows, 4 * half), BF16),
            pltpu.SemaphoreType.DMA((6,)),
            pltpu.SemaphoreType.DMA((sends,)),
            pltpu.SemaphoreType.DMA((sends,)),
        ],
        compiler_params=pltpu.CompilerParams(
            collective_id=0, has_side_effects=True, vmem_limit_bytes=48 * 1024 * 1024
        ),
    )(*[pltpu.with_memory_space_constraint(x, pltpu.HBM) for x in arrays])


def solution(mesh):
    in_specs = (
        P(None, ("grp", "sub")),
        P(None, ("grp", "sub")),
        P(None, "sub"),
        P(None, None, "sub"),
        P(None, "sub"),
        P("sub"),
    )
    out_specs = P(None, ("grp", "sub"))
    return jax.shard_map(
        functools.partial(body, mesh.shape["grp"], mesh.shape["sub"]),
        mesh=mesh,
        in_specs=in_specs,
        out_specs=out_specs,
        check_vma=False,
    )
```

```python
import functools

import jax
import jax.numpy as jnp
from jax import lax
from jax.experimental import pallas as pl
from jax.experimental.pallas import tpu as pltpu
from jax.sharding import PartitionSpec as P

CI = 1024
LANES = 128
TILE = 512
SUB = 8
CORES = 2
F32 = jnp.float32
BF16 = jnp.bfloat16
NT = (((1,), (1,)), ((), ()))
MESH = pl.DeviceIdType.MESH


def lane_hots(index):
    wide = lax.broadcasted_iota(jnp.int32, (LANES, index.shape[1]), 0)
    return jnp.where(wide == (index & (LANES - 1)), 1.0, 0.0).astype(BF16)


def turned_hots(index):
    square = (LANES, LANES)
    turned = jnp.transpose(jnp.broadcast_to(index & (LANES - 1), square))
    return jnp.where(lax.broadcasted_iota(jnp.int32, square, 1) == turned, 1.0, 0.0).astype(BF16)


def row_hots(index, rows):
    wide = lax.broadcasted_iota(jnp.int32, (2 * rows, index.shape[1]), 0)
    wide = wide // (2 * SUB) * SUB + (wide & (SUB - 1))
    return jnp.where(wide == index // LANES, 1.0, 0.0).astype(BF16)


def twice(value):
    high = value.astype(BF16).astype(F32)
    return high, value - high


def stacked(high, low):
    shape = (SUB, high.shape[1])
    both = jnp.concatenate([jnp.broadcast_to(high, shape), jnp.broadcast_to(low, shape)], axis=0)
    return both.astype(BF16)


def placed(values, row_hot):
    parts = []
    for value in values:
        for at in range(0, row_hot.shape[0], 2 * SUB):
            parts.append(row_hot[at : at + 2 * SUB] * value)
    return jnp.concatenate(parts, axis=0)


def merged(total, rows):
    total = total.reshape(3 * rows // SUB, 2, SUB, LANES)
    return (total[:, 0] + total[:, 1]).reshape(3, rows, LANES)


def gather(ref, lane, row):
    found = [jnp.zeros((SUB, LANES), F32) for _ in range(3)]
    for r in range(ref.shape[1]):
        here = row == r
        for d in range(3):
            line = jnp.broadcast_to(ref[d, r : r + 1, :], (SUB, LANES))
            found[d] = jnp.where(here, jnp.take_along_axis(line, lane, axis=1), found[d])
    return found


def down(value):
    return jnp.sum(value.reshape(-1, LANES), axis=0, keepdims=True)


def whole(row):
    return jnp.sum(row, axis=1, keepdims=True)


class Kernel:
    def __init__(self, refs, rows, nodes, own, shared, groups, columns):
        for name, ref in refs.items():
            setattr(self, name, ref)
        self.rows, self.nodes, self.own, self.shared = rows, nodes, own, shared
        self.groups, self.columns = groups, columns
        self.g = lax.axis_index("grp")
        self.s = lax.axis_index("sub")
        self.core = lax.rem(self.g, CORES)
        self.chip = self.g - self.core
        self.base = self.s * nodes
        self.slot = self.s * CORES + self.core
        self.all_blocks = self.conn_in.shape[1] // (SUB * LANES)
        self.sent = []
        self.count = 0

    def send(self, src, dst, grp, sub, when=None):
        copy = self.prepare(src, dst, grp, sub, when)
        self.guard(when, copy.start)
        return copy

    def prepare(self, src, dst, grp, sub, when=None):
        at = self.count
        self.count += 1
        copy = pltpu.make_async_remote_copy(
            src_ref=src,
            dst_ref=dst,
            send_sem=self.send_sem.at[at],
            recv_sem=self.recv_sem.at[at],
            device_id={"grp": grp, "sub": sub},
            device_id_type=MESH,
        )
        self.sent.append((copy, when))
        return copy

    def guard(self, when, act):
        if when is None:
            act()
        else:
            pl.when(when)(act)

    def drain(self):
        for copy, when in self.sent:
            self.guard(when, copy.wait_send)
        self.sent = []

    def has_next(self):
        return self.s < self.columns - 1

    def has_prev(self):
        return self.s > 0

    def restrict(self):
        total = jnp.zeros((6 * self.rows, LANES), F32)
        for at in range(0, self.fine.shape[1], TILE):
            values = [stacked(*twice(0.5 * self.fine[d : d + 1, at : at + TILE])) for d in range(3)]
            for k in range(2):
                index = self.nmap[k : k + 1, at : at + TILE] - self.base
                left = placed(values, row_hots(index, self.rows))
                total = total + lax.dot_general(left, lane_hots(index), NT, preferred_element_type=F32)
        return merged(total, self.rows)

    def densify(self):
        for at in range(0, self.fine.shape[1], LANES):
            j = at // LANES
            for k in range(2):
                self.nmap_d[k, j : j + 1] = self.nmap[k : k + 1, at : at + LANES] - self.base
        for at in range(0, self.conn.shape[1], LANES):
            j, cut = at // LANES, slice(at, at + LANES)
            for a in range(4):
                self.conn_d[a, j : j + 1] = self.conn[a : a + 1, cut] - self.base
            for k in range(2):
                self.moduli_d[k, j : j + 1] = self.moduli[k : k + 1, cut]
            for i in range(3):
                line = [self.grads[i, a : a + 1, cut] for a in range(3)]
                for a in range(3):
                    self.grads_d[a, i, j : j + 1] = line[a]
                self.grads_d[3, i, j : j + 1] = -(line[0] + line[1] + line[2])

    def make_hots(self):
        width = self.conn.shape[1]
        for a in range(4):
            for at in range(0, width, TILE):
                index = self.conn[a : a + 1, at : at + TILE] - self.base
                for more in range(0, TILE, LANES):
                    start = a * width + at + more
                    self.lane_hot[start : start + LANES] = turned_hots(index[:, more : more + LANES])
                self.row_hot[:, a * width + at : a * width + at + TILE] = row_hots(index, self.rows)

    def prolong(self, field, out_ref):
        for j in range(0, self.nmap_d.shape[1], SUB):
            both = []
            for k in range(2):
                index = self.nmap_d[k, j : j + SUB]
                both.append(gather(field, index & (LANES - 1), index // LANES))
            for d in range(3):
                mean = 0.5 * (both[0][d] + both[1][d])
                for i in range(SUB):
                    out_ref[d : d + 1, (j + i) * LANES : (j + i + 1) * LANES] = mean[i : i + 1]

    def slopes(self, field, j, slot):
        cut = slice(j, j + SUB)
        grad = [[self.grads_d[a, i, cut] for i in range(3)] for a in range(4)]
        moved = []
        for a in range(4):
            index = self.conn_d[a, cut]
            moved.append(gather(field, index & (LANES - 1), index // LANES))
        h = [[sum(moved[a][i] * grad[a][k] for a in range(4)) for k in range(3)] for i in range(3)]
        for i in range(3):
            for k in range(3):
                self.slope[slot, i, k, cut] = h[i][k]
        return h, grad

    def stresses(self, h, j):
        first = self.moduli_d[0, j : j + SUB]
        second = self.moduli_d[1, j : j + SUB]
        bulk = first * (h[0][0] + h[1][1] + h[2][2])
        stress = [[second * (h[i][k] + h[k][i]) for k in range(3)] for i in range(3)]
        for i in range(3):
            stress[i][i] = stress[i][i] + bulk
        return stress, sum(stress[i][k] * h[i][k] for i in range(3) for k in range(3))

    def strains(self, field, j, slot):
        h, grad = self.slopes(field, j, slot)
        stress, power = self.stresses(h, j)
        nodal = []
        for a in range(4):
            nodal.append([twice(sum(stress[i][k] * grad[a][k] for k in range(3))) for i in range(3)])
        return power, nodal

    def branches(self, act):
        count = self.conn_d.shape[1] // SUB
        few = self.all_blocks - count
        for core, first in ((1, 0), (0, count - few)):
            pl.when(self.core == core)(functools.partial(act, range(first * SUB, count * SUB, SUB)))

    def energy(self, c1, c2, blocks):
        total = jnp.zeros((SUB, LANES), F32)
        for j in blocks:
            cut = slice(j, j + SUB)
            h = [
                [
                    self.slope[0, i, k, cut] - c1 * self.slope[1, i, k, cut] + c2 * self.slope[2, i, k, cut]
                    for k in range(3)
                ]
                for i in range(3)
            ]
            total = total + self.stresses(h, j)[1]
        return down(total)

    def hold(self, nodal, block):
        cut = slice(block, block + SUB)
        for a in range(4):
            for d in range(3):
                for k in range(2):
                    self.nodal[a, d, k, cut] = nodal[a][d][k]

    def spread(self, block, total):
        width = self.conn.shape[1]
        tile = TILE // LANES
        for a in range(4):
            for at in range(block, block + SUB, tile):
                values = []
                for d in range(3):
                    high, low = self.nodal.at[a, d, 0], self.nodal.at[a, d, 1]
                    pieces = [stacked(high[j : j + 1], low[j : j + 1]) for j in range(at, at + tile)]
                    values.append(jnp.concatenate(pieces, axis=1))
                cut = slice(a * width + at * LANES, a * width + at * LANES + TILE)
                left = placed(values, self.row_hot[:, cut])
                total = total + jnp.dot(left, self.lane_hot[cut], preferred_element_type=F32)
        return total

    def apply(self, field, slot, blocks, between=None):
        total = jnp.zeros((6 * self.rows, LANES), F32)
        power, held = None, None
        for block in blocks:
            more, nodal = self.strains(field, block, slot)
            power = more if power is None else power + more
            self.hold(nodal, block)
            if held is not None:
                total = self.spread(held, total)
            held = block
        if between is not None:
            between(down(power))
        return merged(self.spread(held, total), self.rows)

    def weighted(self, field):
        return 0.5 * self.mass[...][None] * field[:, : self.own]

    def keep(self, field, forces, phase):
        own = self.own
        self.force[phase, :, :own] = forces[:, :own] + self.weighted(field)
        self.force[phase, :, own:] = forces[:, own:]

    def exchange_forces(self, phase):
        own, shared = self.own, self.shared
        f_ref = self.force.at[phase]
        copies = []
        nxt, prv = self.has_next(), self.has_prev()
        for j in range(CORES):
            grp = self.chip + lax.rem(self.core + j, CORES)
            up = self.send(f_ref.at[:, pl.ds(own, shared)], self.h_prev.at[phase, j], grp, self.s + 1, nxt)
            copies.append((up, prv))
            dn = self.send(f_ref.at[:, pl.ds(0, shared)], self.h_next.at[phase, j], grp, self.s - 1, prv)
            copies.append((dn, nxt))
        grp = self.chip + 1 - self.core
        copies.append((self.send(f_ref, self.h_own.at[phase], grp, self.s), None))
        return copies

    def collect(self, copies):
        for copy, when in copies:
            self.guard(when, copy.wait_recv)

    def join(self, field, before, after):
        own, shared = self.own, self.shared
        return jnp.concatenate(
            [field[:, :shared] + before, field[:, shared:own], field[:, own:] + after], axis=1
        )

    def joined_forces(self, phase):
        both = self.force[phase] + self.h_own[phase]
        return self.join(
            both,
            self.h_prev[phase, 0] + self.h_prev[phase, 1],
            self.h_next[phase, 0] + self.h_next[phase, 1],
        )

    def share(self, buf):
        copies = []
        for k in range(self.columns):
            for j in range(CORES):
                if k or j:
                    sub = lax.rem(self.s + k, self.columns)
                    grp = self.chip + lax.rem(self.core + j, CORES)
                    copies.append((self.prepare(buf.at[self.slot], buf.at[self.slot], grp, sub), None))
        return copies

    def total(self, buf):
        return sum(buf[i] for i in range(self.columns * CORES))

    def run(self):
        own, shared, rows, G = self.own, self.shared, self.rows, self.groups
        g, s = self.g, self.s
        nxt, prv = self.has_next(), self.has_prev()
        half = self.conn.shape[1]
        at = pl.multiple_of((1 - self.core) * (self.conn_in.shape[1] - half), LANES)
        loads = []
        pairs = [
            (self.nmap_in, self.nmap),
            (self.fine_in, self.fine),
            (self.conn_in.at[:, pl.ds(at, half)], self.conn),
            (self.grads_in.at[:, :, pl.ds(at, half)], self.grads),
            (self.moduli_in.at[:, pl.ds(at, half)], self.moduli),
            (self.mass_in, self.mass),
        ]
        for i, (src, dst) in enumerate(pairs):
            copy = pltpu.make_async_copy(src, dst, self.load_sem.at[i])
            copy.start()
            loads.append(copy)

        barrier = pltpu.get_barrier_semaphore()

        def greet(grp, sub, when=None):
            def act():
                pl.semaphore_signal(barrier, inc=1, device_id={"grp": grp, "sub": sub}, device_id_type=MESH)

            self.guard(when, act)

        ends = self.columns >= 8
        edge = jnp.logical_or(s < 2, s >= self.columns - 2)
        for k in range(self.columns):
            sub = lax.rem(s + k, self.columns)
            meets = None
            if ends and k:
                meets = jnp.logical_not(jnp.logical_and(edge, s + sub == self.columns - 1))
            for j in range(CORES):
                if k or j:
                    greet(self.chip + lax.rem(self.core + j, CORES), sub, meets)
        for j in range(CORES, G):
            grp = lax.rem(self.chip + j, G)
            greet(grp, s)
            greet(grp, s + 1, nxt)
            greet(grp, s - 1, prv)

        @pl.when(jnp.logical_not(prv))
        def _():
            self.r_prev[...] = jnp.zeros_like(self.r_prev)
            self.h_prev[...] = jnp.zeros_like(self.h_prev)

        @pl.when(jnp.logical_not(nxt))
        def _():
            self.r_next[...] = jnp.zeros_like(self.r_next)
            self.h_next[...] = jnp.zeros_like(self.h_next)

        loads[0].wait()
        loads[1].wait()
        self.part[...] = self.restrict()
        far = G - CORES
        missed = edge.astype(jnp.int32) if ends else 0
        pl.semaphore_wait(
            barrier,
            self.columns * CORES - 1 - CORES * missed + far + far * (nxt.astype(jnp.int32) + prv.astype(jnp.int32)),
        )
        twin = self.send(self.part, self.r_own.at[0], self.chip + 1 - self.core, s)
        copies = []
        for j in range(G - 1, -1, -1):
            grp = lax.rem(self.chip + self.core + j, G)
            up = self.send(self.part.at[:, pl.ds(own, shared)], self.r_prev.at[j], grp, s + 1, nxt)
            copies.append((up, prv))
            dn = self.send(self.part.at[:, pl.ds(0, shared)], self.r_next.at[j], grp, s - 1, prv)
            copies.append((dn, nxt))
        twin.wait_recv()
        self.pair[...] = self.part[...] + self.r_own[0]
        for j in range(1, G // CORES):
            grp = lax.rem(g + CORES * j, G)
            copies.append((self.send(self.pair, self.r_own.at[j], grp, s), None))
        for copy in loads[2:]:
            copy.wait()
        self.densify()
        self.make_hots()
        self.collect(copies)
        r0 = self.join(
            self.pair[...] + sum(self.r_own[j] for j in range(1, G // CORES)),
            sum(self.r_prev[j] for j in range(G)),
            sum(self.r_next[j] for j in range(G)),
        )
        self.res[0] = r0

        def first(blocks):
            self.keep(self.res[0], self.apply(self.res.at[0], 0, blocks), 0)

        self.branches(first)
        copies = self.exchange_forces(0)
        self.prolong(self.res.at[0], self.back.at[0])
        self.collect(copies)
        w0 = self.joined_forces(0)
        self.image[...] = w0
        mine, image = 0.5 * r0[:, :own], w0[:, :own]
        lines = [down(mine * r0[:, :own]), down(mine * image), down(0.5 * image * image)]
        lines.append(down(self.weighted(w0) * image))
        shares = self.share(self.sum1)
        self.sum1[self.slot] = jnp.concatenate(lines, axis=0)

        def second(blocks):
            def early(power):
                self.sum1[self.slot, 3:4] = self.sum1[self.slot, 3:4] + power
                for copy, _ in shares:
                    copy.start()

            self.keep(self.image[...], self.apply(self.image, 1, blocks, early), 1)

        self.branches(second)
        copies = self.exchange_forces(1)
        self.collect(copies)
        q0 = self.joined_forces(1)
        self.twin[...] = q0

        def third(blocks):
            for j in blocks:
                self.slopes(self.twin, j, 2)

        self.branches(third)
        self.collect(shares)
        sums = self.total(self.sum1)
        means = whole(sums)
        gamma0, mu1, mu2, mu3 = (means[i : i + 1] for i in range(4))
        alpha0 = gamma0 / mu1
        square = alpha0 * alpha0
        gamma1 = whole(sums[0:1] - 2.0 * alpha0 * sums[1:2] + square * sums[2:3])
        delta1 = mu1 - 2.0 * alpha0 * mu2 + square * mu3
        beta1 = gamma1 / gamma0
        alpha1 = gamma1 / (delta1 - beta1 * gamma1 / alpha0)
        a, b = alpha0 + alpha1 + alpha1 * beta1, alpha1 * alpha0
        r2 = r0 - a * w0 + b * q0
        mine = r2[:, :own]
        lines = [down(0.5 * mine * mine), down(self.weighted(r2) * mine)]
        shares = self.share(self.sum2)
        self.sum2[self.slot] = jnp.concatenate(lines, axis=0)

        def last(blocks):
            self.sum2[self.slot, 1:2] = self.sum2[self.slot, 1:2] + self.energy(a, b, blocks)

        self.branches(last)
        for copy, _ in shares:
            copy.start()
        self.res[1] = r0 - alpha0 * w0
        self.res[2] = r2
        self.prolong(self.res.at[1], self.back.at[1])
        self.prolong(self.res.at[2], self.back.at[2])
        self.drain()
        over_gamma, over_alpha = 1.0 / gamma1, 1.0 / alpha1
        self.collect(shares)
        means = whole(self.total(self.sum2))
        gamma2, delta2 = means[0:1], means[1:2]
        beta2 = gamma2 * over_gamma
        alpha2 = gamma2 / (delta2 - beta2 * (gamma2 * over_alpha))
        c1 = alpha1 + alpha2 * beta2
        c0 = alpha0 + beta1 * c1
        self.out[...] = c0 * self.back[0] + c1 * self.back[1] + alpha2 * self.back[2]


NAMES = (
    "fine_in",
    "nmap_in",
    "conn_in",
    "grads_in",
    "moduli_in",
    "mass_in",
    "out",
    "fine",
    "nmap",
    "conn",
    "grads",
    "moduli",
    "mass",
    "part",
    "pair",
    "r_own",
    "r_prev",
    "r_next",
    "force",
    "h_own",
    "h_prev",
    "h_next",
    "sum1",
    "sum2",
    "back",
    "res",
    "image",
    "twin",
    "slope",
    "nmap_d",
    "conn_d",
    "grads_d",
    "moduli_d",
    "nodal",
    "lane_hot",
    "row_hot",
    "load_sem",
    "send_sem",
    "recv_sem",
)


def kernel(*refs, **sizes):
    Kernel(dict(zip(NAMES, refs)), **sizes).run()


def body(groups, columns, fine_res, node_map, connect, grads, moduli, mass):
    nodes = mass.shape[0]
    own = nodes // LANES
    shared = CI // LANES
    rows = own + shared
    blocks = connect.shape[1] // (SUB * LANES)
    half = (blocks - max(1, blocks // 4)) * SUB * LANES
    sends = 2 * groups + groups // CORES + 2 * (2 * CORES + 1) + 2 * (columns * CORES - 1)
    vmem = pltpu.VMEM
    arrays = (fine_res, node_map, connect, grads, moduli, mass.reshape(own, LANES))
    halo = (3, shared, LANES)
    full = (3, rows, LANES)
    return pl.pallas_call(
        functools.partial(
            kernel, rows=rows, nodes=nodes, own=own, shared=shared, groups=groups, columns=columns
        ),
        out_shape=jax.ShapeDtypeStruct(fine_res.shape, F32),
        in_specs=[pl.BlockSpec(memory_space=pltpu.HBM)] * 6,
        out_specs=pl.BlockSpec(memory_space=vmem),
        scratch_shapes=[
            vmem(fine_res.shape, F32),
            vmem(node_map.shape, jnp.int32),
            vmem((4, half), jnp.int32),
            vmem((3, 3, half), F32),
            vmem((2, half), F32),
            vmem((own, LANES), F32),
            vmem(full, F32),
            vmem(full, F32),
            vmem((groups // CORES,) + full, F32),
            vmem((groups,) + halo, F32),
            vmem((groups,) + halo, F32),
            vmem((2,) + full, F32),
            vmem((2,) + full, F32),
            vmem((2, CORES) + halo, F32),
            vmem((2, CORES) + halo, F32),
            vmem((columns * CORES, 4, LANES), F32),
            vmem((columns * CORES, 2, LANES), F32),
            vmem((3,) + fine_res.shape, F32),
            vmem((3,) + full, F32),
            vmem(full, F32),
            vmem(full, F32),
            vmem((3, 3, 3, half // LANES, LANES), F32),
            vmem((2, node_map.shape[1] // LANES, LANES), jnp.int32),
            vmem((4, half // LANES, LANES), jnp.int32),
            vmem((4, 3, half // LANES, LANES), F32),
            vmem((2, half // LANES, LANES), F32),
            vmem((4, 3, 2, half // LANES, LANES), F32),
            vmem((4 * half, LANES), BF16),
            vmem((2 * rows, 4 * half), BF16),
            pltpu.SemaphoreType.DMA((6,)),
            pltpu.SemaphoreType.DMA((sends,)),
            pltpu.SemaphoreType.DMA((sends,)),
        ],
        compiler_params=pltpu.CompilerParams(
            collective_id=0, has_side_effects=True, vmem_limit_bytes=48 * 1024 * 1024
        ),
    )(*[pltpu.with_memory_space_constraint(x, pltpu.HBM) for x in arrays])


def solution(mesh):
    in_specs = (
        P(None, ("grp", "sub")),
        P(None, ("grp", "sub")),
        P(None, "sub"),
        P(None, None, "sub"),
        P(None, "sub"),
        P("sub"),
    )
    out_specs = P(None, ("grp", "sub"))
    return jax.shard_map(
        functools.partial(body, mesh.shape["grp"], mesh.shape["sub"]),
        mesh=mesh,
        in_specs=in_specs,
        out_specs=out_specs,
        check_vma=False,
    )
```

```python
import functools

import jax
import jax.numpy as jnp
from jax import lax
from jax.experimental import pallas as pl
from jax.experimental.pallas import tpu as pltpu
from jax.sharding import PartitionSpec as P

CI = 1024
LANES = 128
TILE = 512
SUB = 8
CORES = 2
F32 = jnp.float32
BF16 = jnp.bfloat16
NT = (((1,), (1,)), ((), ()))
MESH = pl.DeviceIdType.MESH


def lane_hots(index):
    wide = lax.broadcasted_iota(jnp.int32, (LANES, index.shape[1]), 0)
    return jnp.where(wide == (index & (LANES - 1)), 1.0, 0.0).astype(BF16)


def turned_hots(index):
    square = (LANES, LANES)
    turned = jnp.transpose(jnp.broadcast_to(index & (LANES - 1), square))
    return jnp.where(lax.broadcasted_iota(jnp.int32, square, 1) == turned, 1.0, 0.0).astype(BF16)


def row_hots(index, rows):
    wide = lax.broadcasted_iota(jnp.int32, (2 * rows, index.shape[1]), 0)
    wide = wide // (2 * SUB) * SUB + (wide & (SUB - 1))
    return jnp.where(wide == index // LANES, 1.0, 0.0).astype(BF16)


def twice(value):
    high = value.astype(BF16).astype(F32)
    return high, value - high


def stacked(high, low):
    shape = (SUB, high.shape[1])
    both = jnp.concatenate([jnp.broadcast_to(high, shape), jnp.broadcast_to(low, shape)], axis=0)
    return both.astype(BF16)


def placed(values, row_hot):
    parts = []
    for value in values:
        for at in range(0, row_hot.shape[0], 2 * SUB):
            parts.append(row_hot[at : at + 2 * SUB] * value)
    return jnp.concatenate(parts, axis=0)


def merged(total, rows):
    total = total.reshape(3 * rows // SUB, 2, SUB, LANES)
    return (total[:, 0] + total[:, 1]).reshape(3, rows, LANES)


def gather(ref, lane, row):
    found = [jnp.zeros((SUB, LANES), F32) for _ in range(3)]
    for r in range(ref.shape[1]):
        here = row == r
        for d in range(3):
            line = jnp.broadcast_to(ref[d, r : r + 1, :], (SUB, LANES))
            found[d] = jnp.where(here, jnp.take_along_axis(line, lane, axis=1), found[d])
    return found


def down(value):
    return jnp.sum(value.reshape(-1, LANES), axis=0, keepdims=True)


def whole(row):
    return jnp.sum(row, axis=1, keepdims=True)


class Kernel:
    def __init__(self, refs, rows, nodes, own, shared, groups, columns):
        for name, ref in refs.items():
            setattr(self, name, ref)
        self.rows, self.nodes, self.own, self.shared = rows, nodes, own, shared
        self.groups, self.columns = groups, columns
        self.g = lax.axis_index("grp")
        self.s = lax.axis_index("sub")
        self.core = lax.rem(self.g, CORES)
        self.chip = self.g - self.core
        self.base = self.s * nodes
        self.slot = self.s * CORES + self.core
        self.all_blocks = self.conn_in.shape[1] // (SUB * LANES)
        self.sent = []
        self.count = 0

    def send(self, src, dst, grp, sub, when=None):
        copy = self.prepare(src, dst, grp, sub, when)
        self.guard(when, copy.start)
        return copy

    def prepare(self, src, dst, grp, sub, when=None):
        at = self.count
        self.count += 1
        copy = pltpu.make_async_remote_copy(
            src_ref=src,
            dst_ref=dst,
            send_sem=self.send_sem.at[at],
            recv_sem=self.recv_sem.at[at],
            device_id={"grp": grp, "sub": sub},
            device_id_type=MESH,
        )
        self.sent.append((copy, when))
        return copy

    def guard(self, when, act):
        if when is None:
            act()
        else:
            pl.when(when)(act)

    def drain(self):
        for copy, when in self.sent:
            self.guard(when, copy.wait_send)
        self.sent = []

    def has_next(self):
        return self.s < self.columns - 1

    def has_prev(self):
        return self.s > 0

    def restrict(self):
        total = jnp.zeros((6 * self.rows, LANES), F32)
        for at in range(0, self.fine.shape[1], TILE):
            values = [stacked(*twice(0.5 * self.fine[d : d + 1, at : at + TILE])) for d in range(3)]
            for k in range(2):
                index = self.nmap[k : k + 1, at : at + TILE] - self.base
                left = placed(values, row_hots(index, self.rows))
                total = total + lax.dot_general(left, lane_hots(index), NT, preferred_element_type=F32)
        return merged(total, self.rows)

    def densify(self):
        for at in range(0, self.fine.shape[1], LANES):
            j = at // LANES
            for k in range(2):
                self.nmap_d[k, j : j + 1] = self.nmap[k : k + 1, at : at + LANES] - self.base
        for at in range(0, self.conn.shape[1], LANES):
            j, cut = at // LANES, slice(at, at + LANES)
            for a in range(4):
                self.conn_d[a, j : j + 1] = self.conn[a : a + 1, cut] - self.base
            for k in range(2):
                self.moduli_d[k, j : j + 1] = self.moduli[k : k + 1, cut]
            for i in range(3):
                line = [self.grads[i, a : a + 1, cut] for a in range(3)]
                for a in range(3):
                    self.grads_d[a, i, j : j + 1] = line[a]
                self.grads_d[3, i, j : j + 1] = -(line[0] + line[1] + line[2])

    def make_hots(self):
        width = self.conn.shape[1]
        for a in range(4):
            for at in range(0, width, TILE):
                index = self.conn[a : a + 1, at : at + TILE] - self.base
                for more in range(0, TILE, LANES):
                    start = a * width + at + more
                    self.lane_hot[start : start + LANES] = turned_hots(index[:, more : more + LANES])
                self.row_hot[:, a * width + at : a * width + at + TILE] = row_hots(index, self.rows)

    def prolong(self, field, out_ref):
        for j in range(0, self.nmap_d.shape[1], SUB):
            both = []
            for k in range(2):
                index = self.nmap_d[k, j : j + SUB]
                both.append(gather(field, index & (LANES - 1), index // LANES))
            for d in range(3):
                mean = 0.5 * (both[0][d] + both[1][d])
                for i in range(SUB):
                    out_ref[d : d + 1, (j + i) * LANES : (j + i + 1) * LANES] = mean[i : i + 1]

    def slopes(self, field, j, slot):
        cut = slice(j, j + SUB)
        grad = [[self.grads_d[a, i, cut] for i in range(3)] for a in range(4)]
        moved = []
        for a in range(4):
            index = self.conn_d[a, cut]
            moved.append(gather(field, index & (LANES - 1), index // LANES))
        h = [[sum(moved[a][i] * grad[a][k] for a in range(4)) for k in range(3)] for i in range(3)]
        for i in range(3):
            for k in range(3):
                self.slope[slot, i, k, cut] = h[i][k]
        return h, grad

    def stresses(self, h, j):
        first = self.moduli_d[0, j : j + SUB]
        second = self.moduli_d[1, j : j + SUB]
        bulk = first * (h[0][0] + h[1][1] + h[2][2])
        stress = [[second * (h[i][k] + h[k][i]) for k in range(3)] for i in range(3)]
        for i in range(3):
            stress[i][i] = stress[i][i] + bulk
        return stress, sum(stress[i][k] * h[i][k] for i in range(3) for k in range(3))

    def strains(self, field, j, slot):
        h, grad = self.slopes(field, j, slot)
        stress, power = self.stresses(h, j)
        nodal = []
        for a in range(4):
            nodal.append([twice(sum(stress[i][k] * grad[a][k] for k in range(3))) for i in range(3)])
        return power, nodal

    def branches(self, act):
        count = self.conn_d.shape[1] // SUB
        few = self.all_blocks - count
        for core, first in ((1, 0), (0, count - few)):
            pl.when(self.core == core)(functools.partial(act, range(first * SUB, count * SUB, SUB)))

    def energy(self, c1, c2, blocks):
        total = jnp.zeros((SUB, LANES), F32)
        for j in blocks:
            cut = slice(j, j + SUB)
            h = [
                [
                    self.slope[0, i, k, cut] - c1 * self.slope[1, i, k, cut] + c2 * self.slope[2, i, k, cut]
                    for k in range(3)
                ]
                for i in range(3)
            ]
            total = total + self.stresses(h, j)[1]
        return down(total)

    def hold(self, nodal, block):
        cut = slice(block, block + SUB)
        for a in range(4):
            for d in range(3):
                for k in range(2):
                    self.nodal[a, d, k, cut] = nodal[a][d][k]

    def spread(self, block, total):
        width = self.conn.shape[1]
        tile = TILE // LANES
        for a in range(4):
            for at in range(block, block + SUB, tile):
                values = []
                for d in range(3):
                    high, low = self.nodal.at[a, d, 0], self.nodal.at[a, d, 1]
                    pieces = [stacked(high[j : j + 1], low[j : j + 1]) for j in range(at, at + tile)]
                    values.append(jnp.concatenate(pieces, axis=1))
                cut = slice(a * width + at * LANES, a * width + at * LANES + TILE)
                left = placed(values, self.row_hot[:, cut])
                total = total + jnp.dot(left, self.lane_hot[cut], preferred_element_type=F32)
        return total

    def apply(self, field, slot, blocks, between=None):
        total = jnp.zeros((6 * self.rows, LANES), F32)
        power, held = None, None
        for block in blocks:
            more, nodal = self.strains(field, block, slot)
            power = more if power is None else power + more
            self.hold(nodal, block)
            if held is not None:
                total = self.spread(held, total)
            held = block
        if between is not None:
            between(down(power))
        return merged(self.spread(held, total), self.rows)

    def weighted(self, field):
        return 0.5 * self.mass[...][None] * field[:, : self.own]

    def keep(self, field, forces, phase):
        own = self.own
        self.force[phase, :, :own] = forces[:, :own] + self.weighted(field)
        self.force[phase, :, own:] = forces[:, own:]

    def exchange_forces(self, phase):
        own, shared = self.own, self.shared
        f_ref = self.force.at[phase]
        copies = []
        nxt, prv = self.has_next(), self.has_prev()
        for j in range(CORES):
            grp = self.chip + lax.rem(self.core + j, CORES)
            up = self.send(f_ref.at[:, pl.ds(own, shared)], self.h_prev.at[phase, j], grp, self.s + 1, nxt)
            copies.append((up, prv))
            dn = self.send(f_ref.at[:, pl.ds(0, shared)], self.h_next.at[phase, j], grp, self.s - 1, prv)
            copies.append((dn, nxt))
        grp = self.chip + 1 - self.core
        copies.append((self.send(f_ref, self.h_own.at[phase], grp, self.s), None))
        return copies

    def collect(self, copies):
        for copy, when in copies:
            self.guard(when, copy.wait_recv)

    def join(self, field, before, after):
        own, shared = self.own, self.shared
        return jnp.concatenate(
            [field[:, :shared] + before, field[:, shared:own], field[:, own:] + after], axis=1
        )

    def joined_forces(self, phase):
        both = self.force[phase] + self.h_own[phase]
        return self.join(
            both,
            self.h_prev[phase, 0] + self.h_prev[phase, 1],
            self.h_next[phase, 0] + self.h_next[phase, 1],
        )

    def share(self, buf):
        copies = []
        for k in range(self.columns):
            for j in range(CORES):
                if k or j:
                    sub = lax.rem(self.s + k, self.columns)
                    grp = self.chip + lax.rem(self.core + j, CORES)
                    copies.append((self.prepare(buf.at[self.slot], buf.at[self.slot], grp, sub), None))
        return copies

    def total(self, buf):
        return sum(buf[i] for i in range(self.columns * CORES))

    def run(self):
        own, shared, rows, G = self.own, self.shared, self.rows, self.groups
        g, s = self.g, self.s
        nxt, prv = self.has_next(), self.has_prev()
        half = self.conn.shape[1]
        at = pl.multiple_of((1 - self.core) * (self.conn_in.shape[1] - half), LANES)
        loads = []
        pairs = [
            (self.nmap_in, self.nmap),
            (self.fine_in, self.fine),
            (self.conn_in.at[:, pl.ds(at, half)], self.conn),
            (self.grads_in.at[:, :, pl.ds(at, half)], self.grads),
            (self.moduli_in.at[:, pl.ds(at, half)], self.moduli),
            (self.mass_in, self.mass),
        ]
        for i, (src, dst) in enumerate(pairs):
            copy = pltpu.make_async_copy(src, dst, self.load_sem.at[i])
            copy.start()
            loads.append(copy)

        barrier = pltpu.get_barrier_semaphore()

        def greet(grp, sub, when=None):
            def act():
                pl.semaphore_signal(barrier, inc=1, device_id={"grp": grp, "sub": sub}, device_id_type=MESH)

            self.guard(when, act)

        ends = self.columns >= 8
        last = self.columns - 1
        edge = jnp.logical_or(s < 2, s >= last - 1)
        for k in range(self.columns):
            sub = lax.rem(s + k, self.columns)
            meets = None
            if ends and k:
                apart = jnp.logical_and(edge, jnp.logical_or(sub < 2, sub >= last - 1))
                meets = jnp.logical_not(jnp.logical_and(apart, jnp.abs(s - sub) > 1))
            for j in range(CORES):
                if k or j:
                    greet(self.chip + lax.rem(self.core + j, CORES), sub, meets)
        for j in range(CORES, G):
            grp = lax.rem(self.chip + j, G)
            greet(grp, s)
            greet(grp, s + 1, nxt)
            greet(grp, s - 1, prv)

        @pl.when(jnp.logical_not(prv))
        def _():
            self.r_prev[...] = jnp.zeros_like(self.r_prev)
            self.h_prev[...] = jnp.zeros_like(self.h_prev)

        @pl.when(jnp.logical_not(nxt))
        def _():
            self.r_next[...] = jnp.zeros_like(self.r_next)
            self.h_next[...] = jnp.zeros_like(self.h_next)

        loads[0].wait()
        loads[1].wait()
        self.part[...] = self.restrict()
        far = G - CORES
        missed = 2 * edge.astype(jnp.int32) if ends else 0
        pl.semaphore_wait(
            barrier,
            self.columns * CORES - 1 - CORES * missed + far + far * (nxt.astype(jnp.int32) + prv.astype(jnp.int32)),
        )
        twin = self.send(self.part, self.r_own.at[0], self.chip + 1 - self.core, s)
        copies = []
        for j in range(G - 1, -1, -1):
            grp = lax.rem(self.chip + self.core + j, G)
            up = self.send(self.part.at[:, pl.ds(own, shared)], self.r_prev.at[j], grp, s + 1, nxt)
            copies.append((up, prv))
            dn = self.send(self.part.at[:, pl.ds(0, shared)], self.r_next.at[j], grp, s - 1, prv)
            copies.append((dn, nxt))
        twin.wait_recv()
        self.pair[...] = self.part[...] + self.r_own[0]
        for j in range(1, G // CORES):
            grp = lax.rem(g + CORES * j, G)
            copies.append((self.send(self.pair, self.r_own.at[j], grp, s), None))
        for copy in loads[2:]:
            copy.wait()
        self.densify()
        self.make_hots()
        self.collect(copies)
        r0 = self.join(
            self.pair[...] + sum(self.r_own[j] for j in range(1, G // CORES)),
            sum(self.r_prev[j] for j in range(G)),
            sum(self.r_next[j] for j in range(G)),
        )
        self.res[0] = r0

        def first(blocks):
            self.keep(self.res[0], self.apply(self.res.at[0], 0, blocks), 0)

        self.branches(first)
        copies = self.exchange_forces(0)
        self.prolong(self.res.at[0], self.back.at[0])
        self.collect(copies)
        w0 = self.joined_forces(0)
        self.image[...] = w0
        shares = self.share(self.sum1)

        def second(blocks):
            def early(power):
                mine, image = self.res[0, :, :own], self.image[:, :own]
                half = 0.5 * image
                lines = [down(0.5 * mine * mine), down(mine * half), down(image * half)]
                lines.append(down(self.weighted(image) * image) + power)
                self.sum1[self.slot] = jnp.concatenate(lines, axis=0)
                for copy, _ in shares:
                    copy.start()

            self.keep(self.image[...], self.apply(self.image, 1, blocks, early), 1)

        self.branches(second)
        copies = self.exchange_forces(1)
        self.collect(copies)
        q0 = self.joined_forces(1)
        self.twin[...] = q0

        def third(blocks):
            for j in blocks:
                self.slopes(self.twin, j, 2)

        self.branches(third)
        self.collect(shares)
        sums = self.total(self.sum1)
        means = whole(sums)
        gamma0, mu1, mu2, mu3 = (means[i : i + 1] for i in range(4))
        alpha0 = gamma0 / mu1
        square = alpha0 * alpha0
        gamma1 = whole(sums[0:1] - 2.0 * alpha0 * sums[1:2] + square * sums[2:3])
        delta1 = mu1 - 2.0 * alpha0 * mu2 + square * mu3
        beta1 = gamma1 / gamma0
        alpha1 = gamma1 / (delta1 - beta1 * gamma1 / alpha0)
        a, b = alpha0 + alpha1 + alpha1 * beta1, alpha1 * alpha0
        r2 = r0 - a * w0 + b * q0
        mine = r2[:, :own]
        lines = [down(0.5 * mine * mine), down(self.weighted(r2) * mine)]
        shares = self.share(self.sum2)
        self.sum2[self.slot] = jnp.concatenate(lines, axis=0)

        def last(blocks):
            self.sum2[self.slot, 1:2] = self.sum2[self.slot, 1:2] + self.energy(a, b, blocks)

        self.branches(last)
        for copy, _ in shares:
            copy.start()
        self.res[1] = r0 - alpha0 * w0
        self.res[2] = r2
        self.prolong(self.res.at[1], self.back.at[1])
        self.prolong(self.res.at[2], self.back.at[2])
        self.drain()
        over_gamma, over_alpha = 1.0 / gamma1, 1.0 / alpha1
        self.collect(shares)
        means = whole(self.total(self.sum2))
        gamma2, delta2 = means[0:1], means[1:2]
        beta2 = gamma2 * over_gamma
        alpha2 = gamma2 / (delta2 - beta2 * (gamma2 * over_alpha))
        c1 = alpha1 + alpha2 * beta2
        c0 = alpha0 + beta1 * c1
        self.out[...] = c0 * self.back[0] + c1 * self.back[1] + alpha2 * self.back[2]


NAMES = (
    "fine_in",
    "nmap_in",
    "conn_in",
    "grads_in",
    "moduli_in",
    "mass_in",
    "out",
    "fine",
    "nmap",
    "conn",
    "grads",
    "moduli",
    "mass",
    "part",
    "pair",
    "r_own",
    "r_prev",
    "r_next",
    "force",
    "h_own",
    "h_prev",
    "h_next",
    "sum1",
    "sum2",
    "back",
    "res",
    "image",
    "twin",
    "slope",
    "nmap_d",
    "conn_d",
    "grads_d",
    "moduli_d",
    "nodal",
    "lane_hot",
    "row_hot",
    "load_sem",
    "send_sem",
    "recv_sem",
)


def kernel(*refs, **sizes):
    Kernel(dict(zip(NAMES, refs)), **sizes).run()


def body(groups, columns, fine_res, node_map, connect, grads, moduli, mass):
    nodes = mass.shape[0]
    own = nodes // LANES
    shared = CI // LANES
    rows = own + shared
    blocks = connect.shape[1] // (SUB * LANES)
    half = (blocks - max(1, blocks // 4)) * SUB * LANES
    sends = 2 * groups + groups // CORES + 2 * (2 * CORES + 1) + 2 * (columns * CORES - 1)
    vmem = pltpu.VMEM
    arrays = (fine_res, node_map, connect, grads, moduli, mass.reshape(own, LANES))
    halo = (3, shared, LANES)
    full = (3, rows, LANES)
    return pl.pallas_call(
        functools.partial(
            kernel, rows=rows, nodes=nodes, own=own, shared=shared, groups=groups, columns=columns
        ),
        out_shape=jax.ShapeDtypeStruct(fine_res.shape, F32),
        in_specs=[pl.BlockSpec(memory_space=pltpu.HBM)] * 6,
        out_specs=pl.BlockSpec(memory_space=vmem),
        scratch_shapes=[
            vmem(fine_res.shape, F32),
            vmem(node_map.shape, jnp.int32),
            vmem((4, half), jnp.int32),
            vmem((3, 3, half), F32),
            vmem((2, half), F32),
            vmem((own, LANES), F32),
            vmem(full, F32),
            vmem(full, F32),
            vmem((groups // CORES,) + full, F32),
            vmem((groups,) + halo, F32),
            vmem((groups,) + halo, F32),
            vmem((2,) + full, F32),
            vmem((2,) + full, F32),
            vmem((2, CORES) + halo, F32),
            vmem((2, CORES) + halo, F32),
            vmem((columns * CORES, 4, LANES), F32),
            vmem((columns * CORES, 2, LANES), F32),
            vmem((3,) + fine_res.shape, F32),
            vmem((3,) + full, F32),
            vmem(full, F32),
            vmem(full, F32),
            vmem((3, 3, 3, half // LANES, LANES), F32),
            vmem((2, node_map.shape[1] // LANES, LANES), jnp.int32),
            vmem((4, half // LANES, LANES), jnp.int32),
            vmem((4, 3, half // LANES, LANES), F32),
            vmem((2, half // LANES, LANES), F32),
            vmem((4, 3, 2, half // LANES, LANES), F32),
            vmem((4 * half, LANES), BF16),
            vmem((2 * rows, 4 * half), BF16),
            pltpu.SemaphoreType.DMA((6,)),
            pltpu.SemaphoreType.DMA((sends,)),
            pltpu.SemaphoreType.DMA((sends,)),
        ],
        compiler_params=pltpu.CompilerParams(
            collective_id=0, has_side_effects=True, vmem_limit_bytes=48 * 1024 * 1024
        ),
    )(*[pltpu.with_memory_space_constraint(x, pltpu.HBM) for x in arrays])


def solution(mesh):
    in_specs = (
        P(None, ("grp", "sub")),
        P(None, ("grp", "sub")),
        P(None, "sub"),
        P(None, None, "sub"),
        P(None, "sub"),
        P("sub"),
    )
    out_specs = P(None, ("grp", "sub"))
    return jax.shard_map(
        functools.partial(body, mesh.shape["grp"], mesh.shape["sub"]),
        mesh=mesh,
        in_specs=in_specs,
        out_specs=out_specs,
        check_vma=False,
    )
```
